8 devices in a mesh: dp: 1 (over z), ep_b: 2 (over y), ep_a: 4 (over x, core).
Axes of the slice: x: 2, y: 2, z: 1, core: 2. Of those that a mesh axis runs over, the one named last changes fastest.
Arguments:
- tokens: bfloat16 [8, 8192, 1280], P(('dp', 'ep_b', 'ep_a'))
- expert_ids: int32 [8, 8192], P(('dp', 'ep_b', 'ep_a'))
- route_order: int32 [8, 8192], P(('dp', 'ep_b', 'ep_a'))
- w_route: bfloat16 [1280, 256], replicated
- expert_keys: bfloat16 [8, 256], replicated
- temperature: float32 [], replicated
- w_in: bfloat16 [8, 1280, 5120], P(('ep_b', 'ep_a'))
- b_in: bfloat16 [8, 5120], P(('ep_b', 'ep_a'))
- w_out: bfloat16 [8, 5120, 1280], P(('ep_b', 'ep_a'))
- b_out: bfloat16 [8, 1280], P(('ep_b', 'ep_a'))
Outputs:
- output: bfloat16 [8, 8192, 1280], P(('dp', 'ep_b', 'ep_a'))
All inputs are finite; a program needn't handle non-finite values.
Results may differ from the reference program's by a relative error of at most 0.0023964.
Values are sent between devices in bfloat16 or wider.
A program may use at most 1 GiB of HBM per device.

```python
import jax
import jax.numpy as jnp
from jax import lax

TOKENS_DEV = 8192
MODEL_DIM = 1280
HIDDEN_DIM = 5120
ROUTER_DIM = 256
NUM_EXPERTS = 8
CAPACITY = 1280
HOT_SPAN = max(1, NUM_EXPERTS // 4)


def draw_routes(route_key):
    key_list = jax.random.split(route_key, 5)
    shape_ids = (NUM_EXPERTS, TOKENS_DEV)
    spread_ids = jax.random.randint(key_list[0], shape_ids, 0, NUM_EXPERTS)
    hot_pick = jax.random.randint(key_list[1], shape_ids, 0, 4) == 0
    hot_base = jax.random.randint(key_list[2], (NUM_EXPERTS, 1), 0, NUM_EXPERTS)
    hot_ids = (hot_base + jax.random.randint(key_list[3], shape_ids, 0, HOT_SPAN)) % NUM_EXPERTS
    expert_ids = jnp.where(hot_pick, hot_ids, spread_ids).astype(jnp.int32)
    order_keys = jax.random.split(key_list[4], NUM_EXPERTS)
    route_order = jax.vmap(lambda order_key: jax.random.permutation(order_key, TOKENS_DEV))(order_keys)
    return expert_ids, route_order.astype(jnp.int32)


def setup_inputs(seed: int = 0, part: int = 0) -> dict:
    shared_keys = jax.random.split(jax.random.key(seed), 7)
    part_keys = jax.random.split(jax.random.fold_in(jax.random.key(seed + 1), part), 3)
    w_route = jax.random.normal(shared_keys[0], (MODEL_DIM, ROUTER_DIM), jnp.float32) * MODEL_DIM ** -0.5
    expert_keys = jax.random.normal(shared_keys[1], (NUM_EXPERTS, ROUTER_DIM), jnp.float32)
    temperature = jax.random.uniform(shared_keys[2], (), jnp.float32, 0.1, 0.16)
    w_in = jax.random.normal(shared_keys[3], (NUM_EXPERTS, MODEL_DIM, HIDDEN_DIM), jnp.float32) * MODEL_DIM ** -0.5
    b_in = jax.random.normal(shared_keys[4], (NUM_EXPERTS, HIDDEN_DIM), jnp.float32) * 0.5
    w_out = jax.random.normal(shared_keys[5], (NUM_EXPERTS, HIDDEN_DIM, MODEL_DIM), jnp.float32) * HIDDEN_DIM ** -0.5
    b_out = jax.random.normal(shared_keys[6], (NUM_EXPERTS, MODEL_DIM), jnp.float32) * 0.5
    expert_ids, route_order = draw_routes(part_keys[0])
    key_proj = jnp.dot(expert_keys, w_route.T)
    noise_rows = jax.random.normal(part_keys[1], (NUM_EXPERTS, TOKENS_DEV, MODEL_DIM), jnp.float32)
    strength = jax.random.uniform(part_keys[2], (NUM_EXPERTS, TOKENS_DEV, 1), jnp.float32, 0.5, 1.5)
    tokens = noise_rows + strength * key_proj[expert_ids]
    return {
        "tokens": tokens.astype(jnp.bfloat16),
        "expert_ids": expert_ids,
        "route_order": route_order,
        "w_route": w_route.astype(jnp.bfloat16),
        "expert_keys": expert_keys.astype(jnp.bfloat16),
        "temperature": temperature,
        "w_in": w_in.astype(jnp.bfloat16),
        "b_in": b_in.astype(jnp.bfloat16),
        "w_out": w_out.astype(jnp.bfloat16),
        "b_out": b_out.astype(jnp.bfloat16),
    }


def device_route(tok_rows, id_row, order_row, w_route, key_unit, temperature):
    projected = jnp.dot(tok_rows, w_route, preferred_element_type=jnp.float32)
    proj_unit = projected / jnp.sqrt(jnp.sum(projected * projected, axis=1, keepdims=True))
    router_prob = jax.nn.softmax(jnp.dot(proj_unit, key_unit.T) / temperature, axis=1)
    gate_prob = jnp.take_along_axis(router_prob, id_row[:, None], axis=1)[:, 0]
    ranked_ids = id_row[order_row]
    ranked_hot = (ranked_ids[:, None] == jnp.arange(NUM_EXPERTS)[None, :]).astype(jnp.int32)
    ranked_pos = jnp.sum(jnp.cumsum(ranked_hot, axis=0) * ranked_hot, axis=1) - 1
    slot_pos = jnp.zeros((TOKENS_DEV,), jnp.int32).at[order_row].set(ranked_pos)
    dest_slot = jnp.where(slot_pos < CAPACITY, id_row * CAPACITY + slot_pos, NUM_EXPERTS * CAPACITY)
    send_rows = jnp.zeros((NUM_EXPERTS * CAPACITY, MODEL_DIM), jnp.bfloat16).at[dest_slot].set(tok_rows, mode="drop")
    return send_rows, gate_prob, dest_slot


def expert_apply(operands):
    slot_rows, w_first, b_first, w_second, b_second = operands
    hidden = jnp.dot(slot_rows, w_first, preferred_element_type=jnp.float32) + b_first.astype(jnp.float32)
    hidden = jax.nn.gelu(hidden, approximate=False).astype(jnp.bfloat16)
    result = jnp.dot(hidden, w_second, preferred_element_type=jnp.float32) + b_second.astype(jnp.float32)
    return result.astype(jnp.bfloat16)


def reference(tokens, expert_ids, route_order, w_route, expert_keys, temperature, w_in, b_in, w_out, b_out):
    keys_f32 = expert_keys.astype(jnp.float32)
    key_unit = keys_f32 / jnp.sqrt(jnp.sum(keys_f32 * keys_f32, axis=1, keepdims=True))

    def route_one(operands):
        tok_rows, id_row, order_row = operands
        return device_route(tok_rows, id_row, order_row, w_route, key_unit, temperature)

    send_rows, gate_prob, dest_slot = lax.map(route_one, (tokens, expert_ids, route_order))
    grid_rows = send_rows.reshape(NUM_EXPERTS, NUM_EXPERTS, CAPACITY, MODEL_DIM)
    arrived = jnp.swapaxes(grid_rows, 0, 1).reshape(NUM_EXPERTS, NUM_EXPERTS * CAPACITY, MODEL_DIM)
    expert_out = lax.map(expert_apply, (arrived, w_in, b_in, w_out, b_out))
    returned = jnp.swapaxes(expert_out.reshape(NUM_EXPERTS, NUM_EXPERTS, CAPACITY, MODEL_DIM), 0, 1)
    returned = returned.reshape(NUM_EXPERTS, NUM_EXPERTS * CAPACITY, MODEL_DIM)

    def combine_one(operands):
        back_rows, dest_row, gate_row = operands
        picked = jnp.take(back_rows, dest_row, axis=0, mode="fill", fill_value=0)
        return (gate_row[:, None] * picked.astype(jnp.float32)).astype(jnp.bfloat16)

    return lax.map(combine_one, (returned, dest_slot, gate_prob))
```

```python
import functools

import jax
import jax.numpy as jnp
from jax import lax
from jax.experimental import pallas as pl
from jax.experimental.pallas import tpu as pltpu
from jax.sharding import PartitionSpec as P

EXPERT_AXES = ("ep_b", "ep_a")
CHUNKS = 5
BLK = 256
GRP = 16
WIN = 64
MESH = pl.DeviceIdType.MESH
HID_TILE = 512


def onehot(mask):
    return jnp.where(mask, 1.0, 0.0)


def route_kernel(num_experts, capacity, order_ref, ids_ref, table_ref, code_ref, base_ref, passes_ref, total_ref, hot, keep):
    tok = order_ref.shape[1]
    blocks = tok // BLK
    rows = blocks * num_experts
    expert_col = lax.broadcasted_iota(jnp.int32, (num_experts, BLK), 0)
    lane = lax.broadcasted_iota(jnp.int32, (BLK, BLK), 1)
    sub = lax.broadcasted_iota(jnp.int32, (BLK, BLK), 0)
    before = onehot(sub < lane).astype(jnp.bfloat16)
    ri = lax.broadcasted_iota(jnp.int32, (rows, rows), 0)
    ci = lax.broadcasted_iota(jnp.int32, (rows, rows), 1)
    same_e = (ri % num_experts) == (ci % num_experts)
    earlier_block = onehot(same_e & (ci < ri)).astype(jnp.bfloat16)
    any_block = onehot(same_e).astype(jnp.bfloat16)
    hi_iota = lax.broadcasted_iota(jnp.int32, (tok // 128, BLK), 0)
    lo_iota = lax.broadcasted_iota(jnp.int32, (128, BLK), 0)

    def hi_lo(b):
        order = order_ref[:, b * BLK:(b + 1) * BLK]
        return onehot(hi_iota == (order >> 7)).astype(jnp.bfloat16), onehot(lo_iota == (order & 127))

    def counts(oh):
        count = jnp.sum(oh, axis=1, keepdims=True)
        wide = jnp.broadcast_to(count, (rows, 128)).astype(jnp.bfloat16)
        prior = jnp.dot(earlier_block, wide, preferred_element_type=jnp.float32)
        within = jnp.dot(oh.astype(jnp.bfloat16), before, preferred_element_type=jnp.float32)
        return count, wide, prior, within

    for b in range(blocks):
        hi, lo = hi_lo(b)
        picked = jnp.dot(table_ref[...], hi, preferred_element_type=jnp.float32)
        ranked = jnp.sum(picked * lo, axis=0, keepdims=True).astype(jnp.int32)
        hot[b * num_experts:(b + 1) * num_experts, :] = onehot(expert_col == ranked)
    oh = hot[...]
    _, _, prior, within = counts(oh)
    hot[...] = oh * onehot(within + prior[:, :1] < capacity)
    acc = jnp.zeros((tok // 128, 128), jnp.float32)
    for b in range(blocks):
        hi, lo = hi_lo(b)
        kept = jnp.sum(hot[b * num_experts:(b + 1) * num_experts, :], axis=0, keepdims=True)
        acc += lax.dot_general(hi * kept.astype(jnp.bfloat16), lo.astype(jnp.bfloat16), (((1,), (1,)), ((), ())), preferred_element_type=jnp.float32)
    keep[...] = acc
    for b in range(blocks):
        kept = jnp.concatenate([keep[2 * b:2 * b + 1, :], keep[2 * b + 1:2 * b + 2, :]], axis=1)
        ids = ids_ref[:, b * BLK:(b + 1) * BLK]
        hot[b * num_experts:(b + 1) * num_experts, :] = onehot(expert_col == ids) * onehot(kept > 0.5)
    oh = hot[...]
    count, wide, prior, within = counts(oh)
    total = jnp.dot(any_block, wide, preferred_element_type=jnp.float32)
    start = prior.astype(jnp.int32)
    base = start // GRP
    local = (start - base * GRP)[:, :1]
    within = within.astype(jnp.int32) + local
    expert_row = lax.broadcasted_iota(jnp.int32, (rows, BLK), 0) % num_experts
    code = (within // WIN) * (num_experts * WIN) + expert_row * WIN + within % WIN
    hot[...] = oh * (code + 1).astype(jnp.float32)
    for b in range(blocks):
        one = jnp.sum(hot[b * num_experts:(b + 1) * num_experts, :], axis=0, keepdims=True)
        code_ref[b:b + 1, :] = one.astype(jnp.int32) - 1
    need = (local + count.astype(jnp.int32) + (WIN - 1)) // WIN
    base_ref[...] = base
    passes_ref[...] = jnp.broadcast_to(jnp.where(count > 0.5, need, 0), (rows, 128))
    total_ref[...] = total[:num_experts].astype(jnp.int32)


def route(order_row, id_row, num_experts, capacity):
    tok = order_row.shape[0]
    blocks = tok // BLK
    rows = blocks * num_experts
    table = id_row.reshape(tok // 128, 128).T.astype(jnp.bfloat16)
    small = jax.ShapeDtypeStruct((rows, 128), jnp.int32)
    code, base, need, total = pl.pallas_call(
        functools.partial(route_kernel, num_experts, capacity),
        out_shape=(jax.ShapeDtypeStruct((blocks, BLK), jnp.int32), small, small, jax.ShapeDtypeStruct((num_experts, 128), jnp.int32)),
        scratch_shapes=[pltpu.VMEM((rows, BLK), jnp.float32), pltpu.VMEM((tok // 128, 128), jnp.float32)],
        name="route",
    )(order_row[None], id_row[None], table)
    passes = jnp.max(need[:, 0].reshape(blocks, num_experts), axis=1)
    return code, base[:, 0], passes, total[:, 0]


def dispatch_kernel(num_experts, base_ref, passes_ref, x_ref, code_ref, o_ref):
    b = pl.program_id(0)
    span = WIN // GRP

    @pl.when(b == 0)
    def _():
        o_ref[...] = jnp.zeros_like(o_ref)

    code = code_ref[pl.ds(b, 1), :]
    rows = lax.broadcasted_iota(jnp.int32, (num_experts * WIN, BLK), 0)

    def one_pass(p, carry):
        sel = onehot(rows == code - p * (num_experts * WIN)).astype(jnp.bfloat16)
        win = jnp.dot(sel, x_ref[...], preferred_element_type=jnp.float32).astype(jnp.bfloat16)
        win = win.reshape(num_experts, span, GRP, x_ref.shape[1])
        for e in range(num_experts):
            at = pl.ds(jnp.minimum(base_ref[b * num_experts + e] + p * span, o_ref.shape[1] - span), span)
            o_ref[e, at] += win[e]
        return carry

    lax.fori_loop(0, passes_ref[b], one_pass, 0)


def dispatch(tok_rows, code, base, passes, num_experts, slot_groups):
    tok, width = tok_rows.shape
    size = slot_groups + WIN // GRP
    shape = (num_experts, size, GRP, width)
    return pl.pallas_call(
        functools.partial(dispatch_kernel, num_experts),
        grid_spec=pltpu.PrefetchScalarGridSpec(
            num_scalar_prefetch=2,
            grid=(tok // BLK,),
            in_specs=[
                pl.BlockSpec((BLK, width), lambda i, *_: (i, 0)),
                pl.BlockSpec(code.shape, lambda i, *_: (0, 0)),
            ],
            out_specs=pl.BlockSpec(shape, lambda i, *_: (0, 0, 0, 0), pipeline_mode=pl.Buffered(1)),
        ),
        out_shape=jax.ShapeDtypeStruct(shape, jnp.bfloat16),
        compiler_params=pltpu.CompilerParams(vmem_limit_bytes=48 * 2**20),
        name="dispatch",
    )(base, passes, tok_rows, code)


def partner(d):
    row, col = lax.axis_index("ep_b"), lax.axis_index("ep_a")
    to_row = (row + d // 4) % 2
    to_col = ((col // 2 + (d // 2) % 2) % 2) * 2 + (col % 2 + d % 2) % 2
    return to_row * 4 + to_col, {"ep_b": to_row, "ep_a": to_col}


def exchange_kernel(num_experts, slot_groups, send, w1_hbm, b1_ref, w2_hbm, b2_ref, back, recv, staged, w1, w2, x, y, h, sem_w, sem_x, sem_y, out_s, out_r, ret_s, ret_r):
    cg = slot_groups // CHUNKS
    me, _ = partner(0)

    def to_expert(d, c):
        peer, where = partner(d)
        return pltpu.make_async_remote_copy(send.at[peer, pl.ds(c * cg, cg)], recv.at[d, pl.ds(c * cg, cg)], out_s.at[d, c], out_r.at[d, c], device_id=where, device_id_type=MESH)

    def to_owner(d, c):
        _, where = partner(d)
        return pltpu.make_async_remote_copy(staged.at[d, pl.ds(c * cg, cg)], back.at[me, pl.ds(c * cg, cg)], ret_s.at[d, c], ret_r.at[d, c], device_id=where, device_id_type=MESH)

    barrier = pltpu.get_barrier_semaphore()
    for d in range(1, num_experts):
        pl.semaphore_signal(barrier, inc=1, device_id=partner(d)[1], device_id_type=MESH)
    pl.semaphore_wait(barrier, num_experts - 1)

    far_first = (6, 7, 2, 3, 4, 5, 1)
    for c in range(CHUNKS):
        for d in far_first:
            to_expert(d, c).start()
    load1 = pltpu.make_async_copy(w1_hbm, w1, sem_w.at[0])
    load2 = pltpu.make_async_copy(w2_hbm, w2, sem_w.at[1])
    load1.start()
    load2.start()
    load1.wait()
    load2.wait()

    def step(i, carry):
        c, g = i // (num_experts // 2), i % (num_experts // 2)
        here = pl.ds(c * cg, cg)

        @pl.when(g == 0)
        def _():
            own = pltpu.make_async_copy(send.at[me, here], x.at[0], sem_x.at[0])
            own.start()
            own.wait()

        @pl.when(g != 0)
        def _():
            to_expert(2 * g, c).wait_recv()
            got = pltpu.make_async_copy(recv.at[2 * g, here], x.at[0], sem_x.at[0])
            got.start()
            got.wait()

        to_expert(2 * g + 1, c).wait_recv()
        got = pltpu.make_async_copy(recv.at[2 * g + 1, here], x.at[1], sem_x.at[1])
        got.start()
        got.wait()

        rows = x[...].reshape(2 * cg * GRP, x.shape[3])
        for j in range(w1.shape[1] // HID_TILE):
            cols = pl.ds(j * HID_TILE, HID_TILE)
            pre = jnp.dot(rows, w1[:, cols], preferred_element_type=jnp.float32) + b1_ref[:, cols].astype(jnp.float32)
            act = pre * 0.5 * (1.0 + lax.erf(pre * 0.7071067811865476))
            h[:, cols] = act.astype(jnp.bfloat16)
        hidden = h[...]
        for j in range(w2.shape[1] // 256):
            cols = pl.ds(j * 256, 256)
            res = jnp.dot(hidden, w2[:, cols], preferred_element_type=jnp.float32) + b2_ref[:, cols].astype(jnp.float32)
            y[:, :, :, cols] = res.astype(jnp.bfloat16).reshape(2, cg, GRP, 256)

        @pl.when(g == 0)
        def _():
            own = pltpu.make_async_copy(y.at[0], back.at[me, here], sem_y.at[0])
            own.start()
            own.wait()

        @pl.when(g != 0)
        def _():
            put = pltpu.make_async_copy(y.at[0], staged.at[2 * g, here], sem_y.at[0])
            put.start()
            put.wait()
            to_owner(2 * g, c).start()

        put = pltpu.make_async_copy(y.at[1], staged.at[2 * g + 1, here], sem_y.at[1])
        put.start()
        put.wait()
        to_owner(2 * g + 1, c).start()
        return carry

    lax.fori_loop(0, CHUNKS * num_experts // 2, step, 0)
    for c in range(CHUNKS):
        for d in range(1, num_experts):
            to_expert(d, c).wait_send()
            to_owner(d, c).wait()


def exchange(send, slot_groups, w_first, b_first, w_second, b_second):
    num_experts, _, _, width = send.shape
    hidden = w_first.shape[1]
    cg = slot_groups // CHUNKS
    land = jax.ShapeDtypeStruct((num_experts, slot_groups, GRP, width), jnp.bfloat16)
    back = jax.ShapeDtypeStruct(send.shape, jnp.bfloat16)
    sems = pltpu.SemaphoreType.DMA((num_experts, CHUNKS))
    hbm = pl.BlockSpec(memory_space=pl.ANY)
    vmem = pl.BlockSpec(memory_space=pltpu.VMEM)
    return pl.pallas_call(
        functools.partial(exchange_kernel, num_experts, slot_groups),
        out_shape=(back, land, land),
        in_specs=[hbm, hbm, vmem, hbm, vmem],
        out_specs=(hbm, hbm, hbm),
        scratch_shapes=[
            pltpu.VMEM((width, hidden), jnp.bfloat16),
            pltpu.VMEM((hidden, width), jnp.bfloat16),
            pltpu.VMEM((2, cg, GRP, width), jnp.bfloat16),
            pltpu.VMEM((2, cg, GRP, width), jnp.bfloat16),
            pltpu.VMEM((2 * cg * GRP, hidden), jnp.bfloat16),
            pltpu.SemaphoreType.DMA((2,)),
            pltpu.SemaphoreType.DMA((2,)),
            pltpu.SemaphoreType.DMA((2,)),
            sems, sems, sems, sems,
        ],
        compiler_params=pltpu.CompilerParams(collective_id=0, has_side_effects=True, vmem_limit_bytes=60 * 2**20),
        name="exchange",
    )(send, w_first, b_first[None], w_second, b_second[None])[0]


def combine_kernel(num_experts, base_ref, passes_ref, total_ref, back_ref, code_ref, gate_ref, o_ref):
    b = pl.program_id(0)
    span = WIN // GRP
    width = o_ref.shape[1]
    code = jnp.transpose(jnp.broadcast_to(code_ref[pl.ds(b, 1), :], (128, BLK)))
    cols = lax.broadcasted_iota(jnp.int32, (BLK, 128), 1)
    row = lax.broadcasted_iota(jnp.int32, (WIN, width), 0)
    gate = gate_ref[...]

    def picked(p):
        sel = jnp.concatenate([onehot(cols + k == code - p * (num_experts * WIN)) for k in range(0, num_experts * WIN, 128)], axis=1)
        wins = []
        for e in range(num_experts):
            at = jnp.minimum(base_ref[b * num_experts + e] + p * span, back_ref.shape[1] - span)
            win = back_ref[e, pl.ds(at, span)].reshape(WIN, width)
            wins.append(jnp.where(row < total_ref[e] - at * GRP, win, jnp.zeros_like(win)))
        return jnp.dot(sel.astype(jnp.bfloat16), jnp.concatenate(wins, axis=0), preferred_element_type=jnp.float32)

    o_ref[...] = (gate * picked(0)).astype(jnp.bfloat16)

    def more(p, carry):
        o_ref[...] += (gate * picked(p)).astype(jnp.bfloat16)
        return carry

    lax.fori_loop(1, passes_ref[b], more, 0)


def combine(back, code, base, passes, total, gate):
    tok, width = gate.shape[0], back.shape[3]
    num_experts = back.shape[0]
    return pl.pallas_call(
        functools.partial(combine_kernel, num_experts),
        grid_spec=pltpu.PrefetchScalarGridSpec(
            num_scalar_prefetch=3,
            grid=(tok // BLK,),
            in_specs=[
                pl.BlockSpec(back.shape, lambda i, *_: (0, 0, 0, 0), pipeline_mode=pl.Buffered(1)),
                pl.BlockSpec(code.shape, lambda i, *_: (0, 0)),
                pl.BlockSpec((BLK, 1), lambda i, *_: (i, 0)),
            ],
            out_specs=pl.BlockSpec((BLK, width), lambda i, *_: (i, 0)),
        ),
        out_shape=jax.ShapeDtypeStruct((tok, width), jnp.bfloat16),
        compiler_params=pltpu.CompilerParams(vmem_limit_bytes=48 * 2**20),
        name="combine",
    )(base, passes, total, back, code, gate)


def gates(tok_rows, id_row, w_route, expert_keys, tau):
    keys_f32 = expert_keys.astype(jnp.float32)
    key_unit = keys_f32 / jnp.sqrt(jnp.sum(keys_f32 * keys_f32, axis=1, keepdims=True))
    projected = jnp.dot(tok_rows, w_route, preferred_element_type=jnp.float32)
    proj_unit = projected / jnp.sqrt(jnp.sum(projected * projected, axis=1, keepdims=True))
    prob = jax.nn.softmax(jnp.dot(proj_unit, key_unit.T) / tau, axis=1)
    expert_range = jnp.arange(expert_keys.shape[0], dtype=jnp.int32)[None, :]
    return jnp.sum(jnp.where(id_row[:, None] == expert_range, prob, 0.0), axis=1, keepdims=True)


def solution(mesh):
    num_experts = mesh.shape["ep_b"] * mesh.shape["ep_a"]
    tok_spec = P(("dp",) + EXPERT_AXES)
    expert_spec = P(EXPERT_AXES)

    def device_step(tokens, expert_ids, route_order, w_route, expert_keys, tau, w_in, b_in, w_out, b_out):
        tok_rows, id_row = tokens[0], expert_ids[0]
        tok, width = tok_rows.shape
        capacity = (5 * tok + 4 * num_experts - 1) // (4 * num_experts)
        slot_groups = -(-capacity // (GRP * CHUNKS)) * CHUNKS
        code, base, passes, total = route(route_order[0], id_row, num_experts, capacity)
        send = dispatch(tok_rows, code, base, passes, num_experts, slot_groups)
        back = exchange(send, slot_groups, w_in[0], b_in[0], w_out[0], b_out[0])
        gate = gates(tok_rows, id_row, w_route, expert_keys, tau)
        return combine(back, code, base, passes, total, gate)[None]

    return jax.shard_map(
        device_step,
        mesh=mesh,
        in_specs=(tok_spec, tok_spec, tok_spec, P(), P(), P(), expert_spec, expert_spec, expert_spec, expert_spec),
        out_specs=tok_spec,
        check_vma=False,
    )
```

```python
import functools

import jax
import jax.numpy as jnp
from jax import lax
from jax.experimental import pallas as pl
from jax.experimental.pallas import tpu as pltpu
from jax.sharding import PartitionSpec as P

EXPERT_AXES = ("ep_b", "ep_a")
CHUNKS = 5
BLK = 256
STEP = 4
GRP = 16
UNIT = 8
WIN = 64
MESH = pl.DeviceIdType.MESH
HID_TILE = 512


def onehot(mask):
    return jnp.where(mask, 1.0, 0.0)


def route_kernel(num_experts, capacity, order_ref, ids_ref, grid_ref, code_ref, meta_ref, hot, keep):
    tok = order_ref.shape[1]
    blocks = tok // BLK
    rows = blocks * num_experts
    expert_col = lax.broadcasted_iota(jnp.int32, (num_experts, BLK), 0)
    lane = lax.broadcasted_iota(jnp.int32, (BLK, BLK), 1)
    sub = lax.broadcasted_iota(jnp.int32, (BLK, BLK), 0)
    before = onehot(sub < lane).astype(jnp.bfloat16)
    ri = lax.broadcasted_iota(jnp.int32, (rows, rows), 0)
    ci = lax.broadcasted_iota(jnp.int32, (rows, rows), 1)
    same_e = (ri % num_experts) == (ci % num_experts)
    earlier_block = onehot(same_e & (ci < ri)).astype(jnp.bfloat16)
    any_block = onehot(same_e).astype(jnp.bfloat16)
    hi_iota = lax.broadcasted_iota(jnp.int32, (tok // 128, BLK), 0)
    lo_iota = lax.broadcasted_iota(jnp.int32, (128, BLK), 0)

    def hi_lo(b):
        order = order_ref[:, b * BLK:(b + 1) * BLK]
        return onehot(hi_iota == (order >> 7)).astype(jnp.bfloat16), onehot(lo_iota == (order & 127))

    def counts(oh):
        count = jnp.sum(oh, axis=1, keepdims=True)
        wide = jnp.broadcast_to(count, (rows, 128)).astype(jnp.bfloat16)
        prior = jnp.dot(earlier_block, wide, preferred_element_type=jnp.float32)
        within = jnp.dot(oh.astype(jnp.bfloat16), before, preferred_element_type=jnp.float32)
        return count, wide, prior, within

    table = jnp.transpose(grid_ref[...].astype(jnp.float32)).astype(jnp.bfloat16)
    for b in range(blocks):
        hi, lo = hi_lo(b)
        picked = jnp.dot(table, hi, preferred_element_type=jnp.float32)
        ranked = jnp.sum(picked * lo, axis=0, keepdims=True).astype(jnp.int32)
        hot[b * num_experts:(b + 1) * num_experts, :] = onehot(expert_col == ranked)
    oh = hot[...]
    _, _, prior, within = counts(oh)
    hot[...] = oh * onehot(within + prior[:, :1] < capacity)
    acc = jnp.zeros((tok // 128, 128), jnp.float32)
    for b in range(blocks):
        hi, lo = hi_lo(b)
        kept = jnp.sum(hot[b * num_experts:(b + 1) * num_experts, :], axis=0, keepdims=True)
        acc += lax.dot_general(hi * kept.astype(jnp.bfloat16), lo.astype(jnp.bfloat16), (((1,), (1,)), ((), ())), preferred_element_type=jnp.float32)
    keep[...] = acc
    for b in range(blocks):
        kept = jnp.concatenate([keep[2 * b:2 * b + 1, :], keep[2 * b + 1:2 * b + 2, :]], axis=1)
        ids = ids_ref[:, b * BLK:(b + 1) * BLK]
        hot[b * num_experts:(b + 1) * num_experts, :] = onehot(expert_col == ids) * onehot(kept > 0.5)
    oh = hot[...]
    count, wide, prior, within = counts(oh)
    total = jnp.dot(any_block, wide, preferred_element_type=jnp.float32)
    start = prior.astype(jnp.int32)
    base = start // GRP
    local = (start - base * GRP)[:, :1]
    within = within.astype(jnp.int32) + local
    expert_row = lax.broadcasted_iota(jnp.int32, (rows, BLK), 0) % num_experts
    code = (within // WIN) * (num_experts * WIN) + expert_row * WIN + within % WIN
    hot[...] = oh * (code + 1).astype(jnp.float32)
    for b in range(blocks):
        one = jnp.sum(hot[b * num_experts:(b + 1) * num_experts, :], axis=0, keepdims=True)
        code_ref[b:b + 1, :] = one.astype(jnp.int32) - 1
    need = jnp.where(count > 0.5, (local + count.astype(jnp.int32) + (WIN - 1)) // WIN, 0)
    for row, value in enumerate((base, need, total, local, local + count.astype(jnp.int32))):
        wide = jnp.broadcast_to(value[:, :1], (rows, 128)).astype(jnp.float32)
        meta_ref[row:row + 1, :] = jnp.transpose(wide)[:1].astype(jnp.int32)


def route(order_row, id_row, num_experts, capacity):
    tok = order_row.shape[0]
    blocks = tok // BLK
    rows = blocks * num_experts
    return pl.pallas_call(
        functools.partial(route_kernel, num_experts, capacity),
        out_shape=(jax.ShapeDtypeStruct((blocks, BLK), jnp.int32), jax.ShapeDtypeStruct((8, rows), jnp.int32)),
        scratch_shapes=[pltpu.VMEM((rows, BLK), jnp.float32), pltpu.VMEM((tok // 128, 128), jnp.float32)],
        name="route",
    )(order_row[None], id_row[None], id_row.reshape(tok // 128, 128))


def most(meta_ref, b, num_experts):
    n = meta_ref[1, b * num_experts]
    for e in range(1, num_experts):
        n = jnp.maximum(n, meta_ref[1, b * num_experts + e])
    return n


def used_units(meta_ref, e):
    return (meta_ref[2, e] + (UNIT * GRP - 1)) // (UNIT * GRP)


def dispatch_kernel(num_experts, meta_ref, x_ref, code_ref, o_ref, acc, sem):
    i, last = pl.program_id(0), pl.num_programs(0) - 1
    span = WIN // GRP
    rows = lax.broadcasted_iota(jnp.int32, (num_experts * WIN, BLK), 0)
    sub = lax.broadcasted_iota(jnp.int32, (GRP, x_ref.shape[1]), 0)

    def block(k, carry):
        b = i * STEP + k
        code = code_ref[pl.ds(b, 1), :]
        x = x_ref[pl.ds(pl.multiple_of(k * BLK, BLK), BLK), :]

        def one_pass(p, carry):
            sel = onehot(rows == code - p * (num_experts * WIN)).astype(jnp.bfloat16)
            win = jnp.dot(sel, x, preferred_element_type=jnp.float32).astype(jnp.bfloat16)
            win = win.reshape(num_experts, span, GRP, x_ref.shape[1])
            for e in range(num_experts):
                at = jnp.minimum(meta_ref[0, b * num_experts + e] + p * span, acc.shape[1] - span)
                old = jnp.where(p == 0, meta_ref[3, b * num_experts + e], 0)
                acc[e, at] = jnp.where(sub < old, acc[e, at], win[e, 0])
                acc[e, pl.ds(at + 1, span - 1)] = win[e, 1:]
            return carry

        return lax.fori_loop(0, most(meta_ref, b, num_experts), one_pass, carry)

    lax.fori_loop(0, STEP, block, 0)

    def unit(e, u):
        part = pl.ds(u * UNIT, UNIT)
        return pltpu.make_async_copy(acc.at[e, part], o_ref.at[e, part], sem.at[e, u])

    here, nxt = i * STEP, jnp.minimum(i + 1, last) * STEP
    for e in range(num_experts):
        done = jnp.where(i == last, used_units(meta_ref, e), meta_ref[0, nxt * num_experts + e] // UNIT)
        lax.fori_loop(meta_ref[0, here * num_experts + e] // UNIT, done, lambda u, c, e=e: (unit(e, u).start(), c)[1], 0)

    @pl.when(i == last)
    def _():
        for e in range(num_experts):
            lax.fori_loop(0, used_units(meta_ref, e), lambda u, c, e=e: (unit(e, u).wait(), c)[1], 0)


def dispatch(tok_rows, code, meta, num_experts, slot_groups):
    tok, width = tok_rows.shape
    padded = slot_groups + WIN // GRP
    return pl.pallas_call(
        functools.partial(dispatch_kernel, num_experts),
        grid_spec=pltpu.PrefetchScalarGridSpec(
            num_scalar_prefetch=1,
            grid=(tok // (BLK * STEP),),
            in_specs=[
                pl.BlockSpec((STEP * BLK, width), lambda i, *_: (i, 0)),
                pl.BlockSpec(code.shape, lambda i, *_: (0, 0)),
            ],
            out_specs=pl.BlockSpec(memory_space=pl.ANY),
            scratch_shapes=[
                pltpu.VMEM((num_experts, padded, GRP, width), jnp.bfloat16),
                pltpu.SemaphoreType.DMA((num_experts, slot_groups // UNIT)),
            ],
        ),
        out_shape=jax.ShapeDtypeStruct((num_experts, slot_groups, GRP, width), jnp.bfloat16),
        compiler_params=pltpu.CompilerParams(vmem_limit_bytes=48 * 2**20),
        name="dispatch",
    )(meta, tok_rows, code)


def partner(d):
    row, col = lax.axis_index("ep_b"), lax.axis_index("ep_a")
    to_row = (row + d // 4) % 2
    to_col = ((col // 2 + (d // 2) % 2) % 2) * 2 + (col % 2 + d % 2) % 2
    return to_row * 4 + to_col, {"ep_b": to_row, "ep_a": to_col}


def exchange_kernel(num_experts, slot_groups, send, w1_hbm, b1_ref, w2_hbm, b2_ref, tokens, wr_ref, keys_ref, tau_ref, back, recv, staged, probs, w1, w2, x, y, h, prob, sem_w, sem_x, sem_y, out_s, out_r, ret_s, ret_r):
    cg = slot_groups // CHUNKS
    me, _ = partner(0)

    def to_expert(d, c):
        peer, where = partner(d)
        return pltpu.make_async_remote_copy(send.at[peer, pl.ds(c * cg, cg)], recv.at[d, pl.ds(c * cg, cg)], out_s.at[d, c], out_r.at[d, c], device_id=where, device_id_type=MESH)

    def to_owner(d, c):
        _, where = partner(d)
        return pltpu.make_async_remote_copy(staged.at[d, pl.ds(c * cg, cg)], back.at[me, pl.ds(c * cg, cg)], ret_s.at[d, c], ret_r.at[d, c], device_id=where, device_id_type=MESH)

    barrier = pltpu.get_barrier_semaphore()
    for d in range(1, num_experts):
        pl.semaphore_signal(barrier, inc=1, device_id=partner(d)[1], device_id_type=MESH)
    pl.semaphore_wait(barrier, num_experts - 1)

    far_first = (6, 7, 2, 3, 4, 5, 1)
    for c in range(CHUNKS):
        for d in far_first:
            to_expert(d, c).start()
    load1 = pltpu.make_async_copy(w1_hbm, w1, sem_w.at[0])
    load2 = pltpu.make_async_copy(w2_hbm, w2, sem_w.at[1])
    load1.start()
    load2.start()
    load1.wait()
    load2.wait()

    def step(i, carry):
        c, g = i // (num_experts // 2), i % (num_experts // 2)
        here = pl.ds(c * cg, cg)

        @pl.when(g == 0)
        def _():
            own = pltpu.make_async_copy(send.at[me, here], x.at[0], sem_x.at[0])
            own.start()
            own.wait()

        @pl.when(g != 0)
        def _():
            to_expert(2 * g, c).wait_recv()
            got = pltpu.make_async_copy(recv.at[2 * g, here], x.at[0], sem_x.at[0])
            got.start()
            got.wait()

        to_expert(2 * g + 1, c).wait_recv()
        got = pltpu.make_async_copy(recv.at[2 * g + 1, here], x.at[1], sem_x.at[1])
        got.start()
        got.wait()

        rows = x[...].reshape(2 * cg * GRP, x.shape[3])
        for j in range(w1.shape[1] // HID_TILE):
            cols = pl.ds(j * HID_TILE, HID_TILE)
            pre = jnp.dot(rows, w1[:, cols], preferred_element_type=jnp.float32) + b1_ref[:, cols].astype(jnp.float32)
            act = pre * 0.5 * (1.0 + lax.erf(pre * 0.7071067811865476))
            h[:, cols] = act.astype(jnp.bfloat16)
        hidden = h[...]
        for j in range(w2.shape[1] // 256):
            cols = pl.ds(j * 256, 256)
            res = jnp.dot(hidden, w2[:, cols], preferred_element_type=jnp.float32) + b2_ref[:, cols].astype(jnp.float32)
            y[:, :, :, cols] = res.astype(jnp.bfloat16).reshape(2, cg, GRP, 256)

        @pl.when(g == 0)
        def _():
            own = pltpu.make_async_copy(y.at[0], back.at[me, here], sem_y.at[0])
            own.start()
            own.wait()

        @pl.when(g != 0)
        def _():
            put = pltpu.make_async_copy(y.at[0], staged.at[2 * g, here], sem_y.at[0])
            put.start()
            put.wait()
            to_owner(2 * g, c).start()

        put = pltpu.make_async_copy(y.at[1], staged.at[2 * g + 1, here], sem_y.at[1])
        put.start()
        put.wait()
        to_owner(2 * g + 1, c).start()
        return carry

    lax.fori_loop(0, CHUNKS * num_experts // 2, step, 0)

    keys = keys_ref[...].astype(jnp.float32)
    unit_keys = keys / jnp.sqrt(jnp.sum(keys * keys, axis=1, keepdims=True))
    unit_keys = jnp.concatenate([unit_keys, jnp.zeros((128 - num_experts, keys.shape[1]), jnp.float32)], axis=0)
    real = lax.broadcasted_iota(jnp.int32, prob.shape, 1) < num_experts

    def gate_step(i, carry):
        for half in range(2):
            got = pltpu.make_async_copy(tokens.at[pl.ds((2 * i + half) * cg, cg)], x.at[half], sem_x.at[half])
            got.start()
            got.wait()
        proj = jnp.dot(x[...].reshape(prob.shape[0], x.shape[3]), wr_ref[...], preferred_element_type=jnp.float32)
        unit = proj / jnp.sqrt(jnp.sum(proj * proj, axis=1, keepdims=True))
        logits = lax.dot_general(unit, unit_keys, (((1,), (1,)), ((), ())), preferred_element_type=jnp.float32) / tau_ref[0, 0]
        top = jnp.max(jnp.where(real, logits, -jnp.inf), axis=1, keepdims=True)
        weight = jnp.where(real, jnp.exp(logits - top), 0.0)
        prob[...] = weight / jnp.sum(weight, axis=1, keepdims=True)
        put = pltpu.make_async_copy(prob, probs.at[pl.ds(i * prob.shape[0], prob.shape[0])], sem_y.at[0])
        put.start()
        put.wait()
        return carry

    lax.fori_loop(0, probs.shape[0] // prob.shape[0], gate_step, 0)
    for c in range(CHUNKS):
        for d in range(1, num_experts):
            to_expert(d, c).wait_send()
            to_owner(d, c).wait()


def exchange(send, w_first, b_first, w_second, b_second, tok_rows, w_route, expert_keys, tau):
    num_experts, slot_groups, _, width = send.shape
    tok = tok_rows.shape[0]
    hidden = w_first.shape[1]
    cg = slot_groups // CHUNKS
    land = jax.ShapeDtypeStruct((num_experts, slot_groups, GRP, width), jnp.bfloat16)
    probs = jax.ShapeDtypeStruct((tok, 128), jnp.float32)
    sems = pltpu.SemaphoreType.DMA((num_experts, CHUNKS))
    hbm = pl.BlockSpec(memory_space=pl.ANY)
    vmem = pl.BlockSpec(memory_space=pltpu.VMEM)
    return pl.pallas_call(
        functools.partial(exchange_kernel, num_experts, slot_groups),
        out_shape=(land, land, land, probs),
        in_specs=[hbm, hbm, vmem, hbm, vmem, hbm, vmem, vmem, pl.BlockSpec(memory_space=pltpu.SMEM)],
        out_specs=(hbm, hbm, hbm, hbm),
        scratch_shapes=[
            pltpu.VMEM((width, hidden), jnp.bfloat16),
            pltpu.VMEM((hidden, width), jnp.bfloat16),
            pltpu.VMEM((2, cg, GRP, width), jnp.bfloat16),
            pltpu.VMEM((2, cg, GRP, width), jnp.bfloat16),
            pltpu.VMEM((2 * cg * GRP, hidden), jnp.bfloat16),
            pltpu.VMEM((2 * cg * GRP, 128), jnp.float32),
            pltpu.SemaphoreType.DMA((2,)),
            pltpu.SemaphoreType.DMA((2,)),
            pltpu.SemaphoreType.DMA((2,)),
            sems, sems, sems, sems,
        ],
        compiler_params=pltpu.CompilerParams(collective_id=0, has_side_effects=True, vmem_limit_bytes=60 * 2**20),
        name="exchange",
    )(send, w_first, b_first[None], w_second, b_second[None], tok_rows.reshape(tok // GRP, GRP, width), w_route, expert_keys, tau.reshape(1, 1))


def combine_kernel(num_experts, meta_ref, back_ref, code_ref, prob_ref, o_ref, rows_in, sem):
    i, last = pl.program_id(0), pl.num_programs(0) - 1
    span = WIN // GRP
    width = o_ref.shape[1]
    cols = lax.broadcasted_iota(jnp.int32, (BLK, 128), 1)
    row = lax.broadcasted_iota(jnp.int32, (WIN, width), 0)

    def unit(e, u):
        part = pl.ds(u * UNIT, UNIT)
        return pltpu.make_async_copy(back_ref.at[e, part], rows_in.at[e, part], sem.at[e, u])

    @pl.when(i == 0)
    def _():
        for u in range(back_ref.shape[1] // UNIT):
            for e in range(num_experts):
                @pl.when(u < used_units(meta_ref, e))
                def _():
                    unit(e, u).start()

    def reach(step, e):
        n = (meta_ref[0, step * STEP * num_experts + e] * GRP + meta_ref[3, step * STEP * num_experts + e] + (UNIT * GRP - 1)) // (UNIT * GRP)
        return n

    for e in range(num_experts):
        end = jnp.where(i == last, used_units(meta_ref, e), reach(jnp.minimum(i + 1, last), e))
        lax.fori_loop(reach(i, e), end, lambda u, c, e=e: (unit(e, u).wait(), c)[1], 0)

    def block(k, carry):
        b = i * STEP + k
        mine = pl.ds(pl.multiple_of(k * BLK, BLK), BLK)
        code = jnp.transpose(jnp.broadcast_to(code_ref[pl.ds(b, 1), :], (128, BLK)))
        expert = (code & (num_experts * WIN - 1)) // WIN
        gate = jnp.sum(jnp.where(cols == expert, prob_ref[mine, :], 0.0), axis=1, keepdims=True)

        def picked(p):
            sel = jnp.concatenate([onehot(cols + k == code - p * (num_experts * WIN)) for k in range(0, num_experts * WIN, 128)], axis=1)
            wins = []
            for e in range(num_experts):
                at = jnp.minimum(meta_ref[0, b * num_experts + e] + p * span, rows_in.shape[1] - span)
                rows = rows_in[e, pl.ds(at, span)].reshape(WIN, width)
                end = meta_ref[0, b * num_experts + e] * GRP + meta_ref[4, b * num_experts + e]
                wins.append(jnp.where(row < end - at * GRP, rows, jnp.zeros_like(rows)))
            return jnp.dot(sel.astype(jnp.bfloat16), jnp.concatenate(wins, axis=0), preferred_element_type=jnp.float32)

        o_ref[mine, :] = (gate * picked(0)).astype(jnp.bfloat16)

        def more(p, carry):
            o_ref[mine, :] += (gate * picked(p)).astype(jnp.bfloat16)
            return carry

        return lax.fori_loop(1, most(meta_ref, b, num_experts), more, carry)

    lax.fori_loop(0, STEP, block, 0)


def combine(back, code, meta, probs):
    tok, width = probs.shape[0], back.shape[3]
    num_experts, slot_groups = back.shape[:2]
    return pl.pallas_call(
        functools.partial(combine_kernel, num_experts),
        grid_spec=pltpu.PrefetchScalarGridSpec(
            num_scalar_prefetch=1,
            grid=(tok // (BLK * STEP),),
            in_specs=[
                pl.BlockSpec(memory_space=pl.ANY),
                pl.BlockSpec(code.shape, lambda i, *_: (0, 0)),
                pl.BlockSpec((STEP * BLK, 128), lambda i, *_: (i, 0)),
            ],
            out_specs=pl.BlockSpec((STEP * BLK, width), lambda i, *_: (i, 0)),
            scratch_shapes=[
                pltpu.VMEM((num_experts, slot_groups + WIN // GRP, GRP, width), jnp.bfloat16),
                pltpu.SemaphoreType.DMA((num_experts, slot_groups // UNIT)),
            ],
        ),
        out_shape=jax.ShapeDtypeStruct((tok, width), jnp.bfloat16),
        compiler_params=pltpu.CompilerParams(vmem_limit_bytes=56 * 2**20),
        name="combine",
    )(meta, back, code, probs)


def solution(mesh):
    num_experts = mesh.shape["ep_b"] * mesh.shape["ep_a"]
    tok_spec = P(("dp",) + EXPERT_AXES)
    expert_spec = P(EXPERT_AXES)

    def device_step(tokens, expert_ids, route_order, w_route, expert_keys, tau, w_in, b_in, w_out, b_out):
        tok_rows, id_row = tokens[0], expert_ids[0]
        tok, width = tok_rows.shape
        capacity = (5 * tok + 4 * num_experts - 1) // (4 * num_experts)
        slot_groups = -(-capacity // (GRP * CHUNKS)) * CHUNKS
        code, meta = route(route_order[0], id_row, num_experts, capacity)
        send = dispatch(tok_rows, code, meta, num_experts, slot_groups)
        back, _, _, probs = exchange(send, w_in[0], b_in[0], w_out[0], b_out[0], tok_rows, w_route, expert_keys, tau)
        return combine(back, code, meta, probs)[None]

    return jax.shard_map(
        device_step,
        mesh=mesh,
        in_specs=(tok_spec, tok_spec, tok_spec, P(), P(), P(), expert_spec, expert_spec, expert_spec, expert_spec),
        out_specs=tok_spec,
        check_vma=False,
    )
```

```python
import functools

import jax
import jax.numpy as jnp
from jax import lax
from jax.experimental import pallas as pl
from jax.experimental.pallas import tpu as pltpu
from jax.sharding import PartitionSpec as P

EXPERT_AXES = ("ep_b", "ep_a")
CHUNKS = 5
BLK = 256
STEP = 4
GRP = 16
UNIT = 8
WIN = 64
MESH = pl.DeviceIdType.MESH
HID_TILE = 512


def onehot(mask):
    return jnp.where(mask, 1.0, 0.0)


def route_kernel(num_experts, capacity, order_ref, ids_ref, grid_ref, code_ref, meta_ref, hot, keep):
    tok = order_ref.shape[1]
    blocks = tok // BLK
    rows = blocks * num_experts
    expert_col = lax.broadcasted_iota(jnp.int32, (num_experts, BLK), 0)
    lane = lax.broadcasted_iota(jnp.int32, (BLK, BLK), 1)
    sub = lax.broadcasted_iota(jnp.int32, (BLK, BLK), 0)
    before = onehot(sub < lane).astype(jnp.bfloat16)
    ri = lax.broadcasted_iota(jnp.int32, (rows, rows), 0)
    ci = lax.broadcasted_iota(jnp.int32, (rows, rows), 1)
    same_e = (ri % num_experts) == (ci % num_experts)
    earlier_block = onehot(same_e & (ci < ri)).astype(jnp.bfloat16)
    any_block = onehot(same_e).astype(jnp.bfloat16)
    hi_iota = lax.broadcasted_iota(jnp.int32, (tok // 128, BLK), 0)
    lo_iota = lax.broadcasted_iota(jnp.int32, (128, BLK), 0)

    def hi_lo(b):
        order = order_ref[:, b * BLK:(b + 1) * BLK]
        return onehot(hi_iota == (order >> 7)).astype(jnp.bfloat16), onehot(lo_iota == (order & 127))

    def counts(oh):
        count = jnp.sum(oh, axis=1, keepdims=True)
        wide = jnp.broadcast_to(count, (rows, 128)).astype(jnp.bfloat16)
        prior = jnp.dot(earlier_block, wide, preferred_element_type=jnp.float32)
        within = jnp.dot(oh.astype(jnp.bfloat16), before, preferred_element_type=jnp.float32)
        return count, wide, prior, within

    table = jnp.transpose(grid_ref[...].astype(jnp.float32)).astype(jnp.bfloat16)
    for b in range(blocks):
        hi, lo = hi_lo(b)
        picked = jnp.dot(table, hi, preferred_element_type=jnp.float32)
        ranked = jnp.sum(picked * lo, axis=0, keepdims=True).astype(jnp.int32)
        hot[b * num_experts:(b + 1) * num_experts, :] = onehot(expert_col == ranked)
    oh = hot[...]
    _, _, prior, within = counts(oh)
    hot[...] = oh * onehot(within + prior[:, :1] < capacity)
    acc = jnp.zeros((tok // 128, 128), jnp.float32)
    for b in range(blocks):
        hi, lo = hi_lo(b)
        kept = jnp.sum(hot[b * num_experts:(b + 1) * num_experts, :], axis=0, keepdims=True)
        acc += lax.dot_general(hi * kept.astype(jnp.bfloat16), lo.astype(jnp.bfloat16), (((1,), (1,)), ((), ())), preferred_element_type=jnp.float32)
    keep[...] = acc
    for b in range(blocks):
        kept = jnp.concatenate([keep[2 * b:2 * b + 1, :], keep[2 * b + 1:2 * b + 2, :]], axis=1)
        ids = ids_ref[:, b * BLK:(b + 1) * BLK]
        hot[b * num_experts:(b + 1) * num_experts, :] = onehot(expert_col == ids) * onehot(kept > 0.5)
    oh = hot[...]
    count, wide, prior, within = counts(oh)
    total = jnp.dot(any_block, wide, preferred_element_type=jnp.float32)
    start = prior.astype(jnp.int32)
    base = start // GRP
    local = (start - base * GRP)[:, :1]
    within = within.astype(jnp.int32) + local
    expert_row = lax.broadcasted_iota(jnp.int32, (rows, BLK), 0) % num_experts
    code = (within // WIN) * (num_experts * WIN) + expert_row * WIN + within % WIN
    hot[...] = oh * (code + 1).astype(jnp.float32)
    for b in range(blocks):
        one = jnp.sum(hot[b * num_experts:(b + 1) * num_experts, :], axis=0, keepdims=True)
        code_ref[b:b + 1, :] = one.astype(jnp.int32) - 1
    need = jnp.where(count > 0.5, (local + count.astype(jnp.int32) + (WIN - 1)) // WIN, 0)
    early = jnp.zeros((1, 1), jnp.float32)
    ahead = onehot(start[:, :1] <= (capacity - UNIT * GRP) // (UNIT * GRP) * (UNIT * GRP))
    for b in range(STEP, blocks, STEP):
        early += jnp.min(ahead[b * num_experts:(b + 1) * num_experts], axis=0, keepdims=True)
    needed = jnp.ones((1, 1), jnp.float32)
    behind = onehot(start[:, :1] < UNIT * GRP)
    for b in range(1, blocks):
        needed += jnp.max(behind[b * num_experts:(b + 1) * num_experts], axis=0, keepdims=True)
    meta_ref[6:7, :] = jnp.broadcast_to(needed, (1, rows)).astype(jnp.int32)
    meta_ref[5:6, :] = jnp.broadcast_to(early, (1, rows)).astype(jnp.int32)
    for row, value in enumerate((base, need, total, local, local + count.astype(jnp.int32))):
        wide = jnp.broadcast_to(value[:, :1], (rows, 128)).astype(jnp.float32)
        meta_ref[row:row + 1, :] = jnp.transpose(wide)[:1].astype(jnp.int32)


def route(order_row, id_row, num_experts, capacity):
    tok = order_row.shape[0]
    blocks = tok // BLK
    rows = blocks * num_experts
    return pl.pallas_call(
        functools.partial(route_kernel, num_experts, capacity),
        out_shape=(jax.ShapeDtypeStruct((blocks, BLK), jnp.int32), jax.ShapeDtypeStruct((8, rows), jnp.int32)),
        scratch_shapes=[pltpu.VMEM((rows, BLK), jnp.float32), pltpu.VMEM((tok // 128, 128), jnp.float32)],
        name="route",
    )(order_row[None], id_row[None], id_row.reshape(tok // 128, 128))


def most(meta_ref, b, num_experts):
    n = meta_ref[1, b * num_experts]
    for e in range(1, num_experts):
        n = jnp.maximum(n, meta_ref[1, b * num_experts + e])
    return n


def used_units(meta_ref, e):
    return (meta_ref[2, e] + (UNIT * GRP - 1)) // (UNIT * GRP)


def place(num_experts, meta_ref, b, code, x, acc):
    span = WIN // GRP
    width = x.shape[1]
    rows = lax.broadcasted_iota(jnp.int32, (num_experts * WIN, BLK), 0)
    sub = lax.broadcasted_iota(jnp.int32, (GRP, width), 0)

    def one_pass(p, carry):
        sel = onehot(rows == code - p * (num_experts * WIN)).astype(jnp.bfloat16)
        win = jnp.dot(sel, x, preferred_element_type=jnp.float32).astype(jnp.bfloat16)
        win = win.reshape(num_experts, span, GRP, width)
        for e in range(num_experts):
            at = jnp.minimum(meta_ref[0, b * num_experts + e] + p * span, acc.shape[1] - span)
            old = jnp.where(p == 0, meta_ref[3, b * num_experts + e], 0)
            acc[e, at] = jnp.where(sub < old, acc[e, at], win[e, 0])
            acc[e, pl.ds(at + 1, span - 1)] = win[e, 1:]
        return carry

    lax.fori_loop(0, most(meta_ref, b, num_experts), one_pass, 0)


def first_kernel(num_experts, meta_ref, x_ref, code_ref, o_ref, acc, ring, sem_x, sem_o):
    blocks = meta_ref[6, 0]
    depth = ring.shape[0]

    def load(b):
        return pltpu.make_async_copy(x_ref.at[pl.ds(pl.multiple_of(b * BLK, BLK), BLK)], ring.at[b % depth], sem_x.at[b % depth])

    for b in range(depth):
        @pl.when(b < blocks)
        def _():
            load(b).start()

    def block(b, carry):
        load(b).wait()
        place(num_experts, meta_ref, b, code_ref[pl.ds(b, 1), :], ring[b % depth], acc)

        @pl.when(b + depth < blocks)
        def _():
            load(b + depth).start()

        return carry

    lax.fori_loop(0, blocks, block, 0)
    outs = [pltpu.make_async_copy(acc.at[e, pl.ds(0, UNIT)], o_ref.at[e], sem_o.at[e]) for e in range(num_experts)]
    for out in outs:
        out.start()
    for out in outs:
        out.wait()


def dispatch_first(tok_rows, code, meta, num_experts):
    width = tok_rows.shape[1]
    depth = 8
    return pl.pallas_call(
        functools.partial(first_kernel, num_experts),
        in_specs=[pl.BlockSpec(memory_space=pltpu.SMEM), pl.BlockSpec(memory_space=pl.ANY), pl.BlockSpec(memory_space=pltpu.VMEM)],
        out_specs=pl.BlockSpec(memory_space=pl.ANY),
        out_shape=jax.ShapeDtypeStruct((num_experts, UNIT, GRP, width), jnp.bfloat16),
        scratch_shapes=[
            pltpu.VMEM((num_experts, UNIT + WIN // GRP, GRP, width), jnp.bfloat16),
            pltpu.VMEM((depth, BLK, width), jnp.bfloat16),
            pltpu.SemaphoreType.DMA((depth,)),
            pltpu.SemaphoreType.DMA((num_experts,)),
        ],
        compiler_params=pltpu.CompilerParams(vmem_limit_bytes=32 * 2**20),
        name="dispatch_first",
    )(meta, tok_rows, code)


def dispatch_kernel(num_experts, meta_ref, x_ref, code_ref, _, o_ref, acc, sem):
    i, last = pl.program_id(0), pl.num_programs(0) - 1

    def block(k, carry):
        b = i * STEP + k
        x = x_ref[pl.ds(pl.multiple_of(k * BLK, BLK), BLK), :]
        place(num_experts, meta_ref, b, code_ref[pl.ds(b, 1), :], x, acc)
        return carry

    lax.fori_loop(0, STEP, block, 0)

    def unit(e, u):
        part = pl.ds(u * UNIT, UNIT)
        return pltpu.make_async_copy(acc.at[e, part], o_ref.at[e, part], sem.at[e, u])

    here, nxt = i * STEP, jnp.minimum(i + 1, last) * STEP
    for e in range(num_experts):
        begin = jnp.maximum(meta_ref[0, here * num_experts + e] // UNIT, 1)
        done = jnp.where(i == last, used_units(meta_ref, e), meta_ref[0, nxt * num_experts + e] // UNIT)
        lax.fori_loop(begin, done, lambda u, c, e=e: (unit(e, u).start(), c)[1], 0)

    @pl.when(i == last)
    def _():
        for e in range(num_experts):
            lax.fori_loop(1, used_units(meta_ref, e), lambda u, c, e=e: (unit(e, u).wait(), c)[1], 0)


def dispatch(tok_rows, code, meta, first, slot_groups):
    tok, width = tok_rows.shape
    num_experts = first.shape[0]
    padded = slot_groups + WIN // GRP
    return pl.pallas_call(
        functools.partial(dispatch_kernel, num_experts),
        grid_spec=pltpu.PrefetchScalarGridSpec(
            num_scalar_prefetch=1,
            grid=(tok // (BLK * STEP),),
            in_specs=[
                pl.BlockSpec((STEP * BLK, width), lambda i, *_: (i, 0)),
                pl.BlockSpec(code.shape, lambda i, *_: (0, 0)),
                pl.BlockSpec(memory_space=pl.ANY),
            ],
            out_specs=pl.BlockSpec(memory_space=pl.ANY),
            scratch_shapes=[
                pltpu.VMEM((num_experts, padded, GRP, width), jnp.bfloat16),
                pltpu.SemaphoreType.DMA((num_experts, slot_groups // UNIT)),
            ],
        ),
        out_shape=jax.ShapeDtypeStruct((num_experts, slot_groups, GRP, width), jnp.bfloat16),
        compiler_params=pltpu.CompilerParams(vmem_limit_bytes=48 * 2**20),
        cost_estimate=pl.CostEstimate(flops=2 * tok * num_experts * WIN * width, bytes_accessed=5 * tok * width, transcendentals=0),
        name="dispatch",
    )(meta, tok_rows, code, first)


def partner(d):
    row, col = lax.axis_index("ep_b"), lax.axis_index("ep_a")
    to_row = (row + d // 4) % 2
    to_col = ((col // 2 + (d // 2) % 2) % 2) * 2 + (col % 2 + d % 2) % 2
    return to_row * 4 + to_col, {"ep_b": to_row, "ep_a": to_col}


def exchange_kernel(num_experts, slot_groups, first, send, w1_hbm, b1_ref, w2_hbm, b2_ref, tokens, wr_ref, keys_ref, tau_ref, back, recv, staged, tail, probs, w1, w2, x, y, h, prob, sem_w, sem_x, sem_y, out_s, out_r, ret_s, ret_r):
    cg = slot_groups // CHUNKS
    units = slot_groups // UNIT
    me, _ = partner(0)

    def to_expert(d, u):
        peer, where = partner(d)
        part = pl.ds(u * UNIT, UNIT)
        return pltpu.make_async_remote_copy(send.at[peer, part], recv.at[d, part], out_s.at[d, u], out_r.at[d, u], device_id=where, device_id_type=MESH)

    def to_owner(d, u):
        _, where = partner(d)
        part = pl.ds(u * UNIT, UNIT)
        return pltpu.make_async_remote_copy(staged.at[d, part], back.at[me, part], ret_s.at[d, u], ret_r.at[d, u], device_id=where, device_id_type=MESH)

    barrier = pltpu.get_barrier_semaphore()
    for d in range(1, num_experts):
        pl.semaphore_signal(barrier, inc=1, device_id=partner(d)[1], device_id_type=MESH)
    pl.semaphore_wait(barrier, num_experts - 1)

    far_first = (6, 7, 2, 3, 4, 5, 1)
    for u in range(1, units):
        for d in far_first:
            to_expert(d, u).start()
    load1 = pltpu.make_async_copy(w1_hbm, w1, sem_w.at[0])
    load2 = pltpu.make_async_copy(w2_hbm, w2, sem_w.at[1])
    load1.start()
    load2.start()
    load1.wait()
    load2.wait()

    def step(i, carry):
        c, g = i // (num_experts // 2), i % (num_experts // 2)
        per = cg // UNIT

        def take(src, half, k):
            return pltpu.make_async_copy(src, x.at[half, pl.ds(k * UNIT, UNIT)], sem_x.at[half, k])

        for half in range(2):
            d = 2 * g + half
            for k in range(per):
                u = c * per + k
                part = pl.ds(u * UNIT, UNIT)

                @pl.when(u == 0)
                def _():
                    take(first.at[partner(d)[0]], half, k).start()

                @pl.when((u != 0) & (d == 0))
                def _():
                    take(send.at[me, part], half, k).start()

                @pl.when((u != 0) & (d != 0))
                def _():
                    to_expert(d, u).wait_recv()
                    take(recv.at[d, part], half, k).start()
        for half in range(2):
            for k in range(per):
                take(first.at[me], half, k).wait()

        rows = x[...].reshape(2 * cg * GRP, x.shape[3])
        for j in range(w1.shape[1] // HID_TILE):
            cols = pl.ds(j * HID_TILE, HID_TILE)
            pre = jnp.dot(rows, w1[:, cols], preferred_element_type=jnp.float32) + b1_ref[:, cols].astype(jnp.float32)
            act = pre * 0.5 * (1.0 + lax.erf(pre * 0.7071067811865476))
            h[:, cols] = act.astype(jnp.bfloat16)
        hidden = h[...]
        for j in range(w2.shape[1] // 256):
            cols = pl.ds(j * 256, 256)
            res = jnp.dot(hidden, w2[:, cols], preferred_element_type=jnp.float32) + b2_ref[:, cols].astype(jnp.float32)
            y[:, :, :, cols] = res.astype(jnp.bfloat16).reshape(2, cg, GRP, 256)

        def put(half, k, dst):
            return pltpu.make_async_copy(y.at[half, pl.ds(k * UNIT, UNIT)], dst, sem_y.at[half, k])

        for half in range(2):
            d = 2 * g + half
            for k in range(per):
                u = c * per + k
                part = pl.ds(u * UNIT, UNIT)

                @pl.when(u == units - 1)
                def _():
                    put(half, k, tail.at[partner(d)[0]]).start()

                @pl.when((u != units - 1) & (d == 0))
                def _():
                    put(half, k, back.at[me, part]).start()

                @pl.when((u != units - 1) & (d != 0))
                def _():
                    put(half, k, staged.at[d, part]).start()

        for half in range(2):
            d = 2 * g + half
            for k in range(per):
                u = c * per + k
                put(half, k, tail.at[me]).wait()

                @pl.when((u != units - 1) & (d != 0))
                def _():
                    to_owner(d, u).start()
        return carry

    lax.fori_loop(0, CHUNKS * num_experts // 2, step, 0)

    keys = keys_ref[...].astype(jnp.float32)
    unit_keys = keys / jnp.sqrt(jnp.sum(keys * keys, axis=1, keepdims=True))
    unit_keys = jnp.concatenate([unit_keys, jnp.zeros((128 - num_experts, keys.shape[1]), jnp.float32)], axis=0)
    real = lax.broadcasted_iota(jnp.int32, prob.shape, 1) < num_experts

    def gate_step(i, carry):
        for half in range(2):
            got = pltpu.make_async_copy(tokens.at[pl.ds((2 * i + half) * cg, cg)], x.at[half], sem_x.at[half, 0])
            got.start()
            got.wait()
        proj = jnp.dot(x[...].reshape(prob.shape[0], x.shape[3]), wr_ref[...], preferred_element_type=jnp.float32)
        unit = proj / jnp.sqrt(jnp.sum(proj * proj, axis=1, keepdims=True))
        logits = lax.dot_general(unit, unit_keys, (((1,), (1,)), ((), ())), preferred_element_type=jnp.float32) / tau_ref[0, 0]
        top = jnp.max(jnp.where(real, logits, -jnp.inf), axis=1, keepdims=True)
        weight = jnp.where(real, jnp.exp(logits - top), 0.0)
        prob[...] = weight / jnp.sum(weight, axis=1, keepdims=True)
        put = pltpu.make_async_copy(prob, probs.at[pl.ds(i * prob.shape[0], prob.shape[0])], sem_y.at[0, 0])
        put.start()
        put.wait()
        return carry

    lax.fori_loop(0, probs.shape[0] // prob.shape[0], gate_step, 0)
    for u in range(1, units):
        for d in range(1, num_experts):
            to_expert(d, u).wait_send()
    for u in range(units - 1):
        for d in range(1, num_experts):
            to_owner(d, u).wait()


def exchange(first, send, w_first, b_first, w_second, b_second, tok_rows, w_route, expert_keys, tau):
    num_experts, slot_groups, _, width = send.shape
    tok = tok_rows.shape[0]
    hidden = w_first.shape[1]
    cg = slot_groups // CHUNKS
    land = jax.ShapeDtypeStruct((num_experts, slot_groups, GRP, width), jnp.bfloat16)
    tail = jax.ShapeDtypeStruct((num_experts, UNIT, GRP, width), jnp.bfloat16)
    probs = jax.ShapeDtypeStruct((tok, 128), jnp.float32)
    sems = pltpu.SemaphoreType.DMA((num_experts, slot_groups // UNIT))
    hbm = pl.BlockSpec(memory_space=pl.ANY)
    vmem = pl.BlockSpec(memory_space=pltpu.VMEM)
    return pl.pallas_call(
        functools.partial(exchange_kernel, num_experts, slot_groups),
        out_shape=(land, land, land, tail, probs),
        in_specs=[hbm, hbm, hbm, vmem, hbm, vmem, hbm, vmem, vmem, pl.BlockSpec(memory_space=pltpu.SMEM)],
        out_specs=(hbm, hbm, hbm, hbm, hbm),
        scratch_shapes=[
            pltpu.VMEM((width, hidden), jnp.bfloat16),
            pltpu.VMEM((hidden, width), jnp.bfloat16),
            pltpu.VMEM((2, cg, GRP, width), jnp.bfloat16),
            pltpu.VMEM((2, cg, GRP, width), jnp.bfloat16),
            pltpu.VMEM((2 * cg * GRP, hidden), jnp.bfloat16),
            pltpu.VMEM((2 * cg * GRP, 128), jnp.float32),
            pltpu.SemaphoreType.DMA((2,)),
            pltpu.SemaphoreType.DMA((2, cg // UNIT)),
            pltpu.SemaphoreType.DMA((2, cg // UNIT)),
            sems, sems, sems, sems,
        ],
        compiler_params=pltpu.CompilerParams(collective_id=0, has_side_effects=True, vmem_limit_bytes=60 * 2**20),
        name="exchange",
    )(first, send, w_first, b_first[None], w_second, b_second[None], tok_rows.reshape(tok // GRP, GRP, width), w_route, expert_keys, tau.reshape(1, 1))


def combine_kernel(num_experts, final, meta_ref, back_ref, tail_ref, code_ref, prob_ref, o_ref, rows_in, sem):
    early = meta_ref[5, 0]
    first = early if final else 0
    i, last = pl.program_id(0), pl.num_programs(0) - 1
    span = WIN // GRP
    width = o_ref.shape[1]
    units = sem.shape[1]
    cols = lax.broadcasted_iota(jnp.int32, (BLK, 128), 1)
    row = lax.broadcasted_iota(jnp.int32, (WIN, width), 0)

    def unit(e, u, from_tail=False):
        part = pl.ds(u * UNIT, UNIT)
        return pltpu.make_async_copy(tail_ref.at[e] if from_tail else back_ref.at[e, part], rows_in.at[e, part], sem.at[e, u])

    def rows_before(step, e):
        n = step * STEP * num_experts + e
        return meta_ref[0, n] * GRP + meta_ref[3, n]

    def reach(step, e):
        return (rows_before(step, e) + (UNIT * GRP - 1)) // (UNIT * GRP)

    def block(k, carry):
        b = i * STEP + k
        mine = pl.ds(pl.multiple_of(k * BLK, BLK), BLK)
        code = jnp.transpose(jnp.broadcast_to(code_ref[pl.ds(b, 1), :], (128, BLK)))
        expert = (code & (num_experts * WIN - 1)) // WIN
        gate = jnp.sum(jnp.where(cols == expert, prob_ref[mine, :], 0.0), axis=1, keepdims=True)

        def picked(p):
            sel = jnp.concatenate([onehot(cols + k == code - p * (num_experts * WIN)) for k in range(0, num_experts * WIN, 128)], axis=1)
            wins = []
            for e in range(num_experts):
                at = jnp.minimum(meta_ref[0, b * num_experts + e] + p * span, rows_in.shape[1] - span)
                rows = rows_in[e, pl.ds(at, span)].reshape(WIN, width)
                end = meta_ref[0, b * num_experts + e] * GRP + meta_ref[4, b * num_experts + e]
                wins.append(jnp.where(row < end - at * GRP, rows, jnp.zeros_like(rows)))
            return jnp.dot(sel.astype(jnp.bfloat16), jnp.concatenate(wins, axis=0), preferred_element_type=jnp.float32)

        o_ref[mine, :] = (gate * picked(0)).astype(jnp.bfloat16)

        def more(p, carry):
            o_ref[mine, :] += (gate * picked(p)).astype(jnp.bfloat16)
            return carry

        return lax.fori_loop(1, most(meta_ref, b, num_experts), more, carry)

    @pl.when(i == first)
    def _():
        for u in range(units if final else units - 1):
            for e in range(num_experts):
                if final:
                    wanted = (u >= rows_before(early, e) // (UNIT * GRP)) & (u < used_units(meta_ref, e))
                else:
                    wanted = u < reach(early, e)

                @pl.when(wanted)
                def _():
                    unit(e, u, u == units - 1).start()

    @pl.when((i >= early) if final else (i < early))
    def _():
        for e in range(num_experts):
            begin = reach(i, e)
            end = reach(jnp.minimum(i + 1, last), e)
            if final:
                begin = jnp.where(i == early, rows_before(early, e) // (UNIT * GRP), begin)
                end = jnp.where(i == last, used_units(meta_ref, e), end)
            lax.fori_loop(begin, end, lambda u, c, e=e: (unit(e, u).wait(), c)[1], 0)
        lax.fori_loop(0, STEP, block, 0)


def combine(back, tail, code, meta, probs, out=None):
    tok, width = probs.shape[0], back.shape[3]
    num_experts, slot_groups = back.shape[:2]
    final = out is not None
    steps = tok // (BLK * STEP)
    kernel = functools.partial(combine_kernel, num_experts, final)
    hbm = pl.BlockSpec(memory_space=pl.ANY)

    def mine(i, meta_ref):
        return (jnp.maximum(i, meta_ref[5, 0]), 0) if final else (jnp.minimum(i, jnp.maximum(meta_ref[5, 0] - 1, 0)), 0)

    def call(meta_ref, *refs):
        if final:
            back_ref, tail_ref, code_ref, prob_ref, _, *rest = refs
        else:
            back_ref, code_ref, prob_ref, *rest = refs
            tail_ref = None
        kernel(meta_ref, back_ref, tail_ref, code_ref, prob_ref, *rest)

    table = pl.BlockSpec(code.shape, lambda i, *_: (0, 0))
    gates = pl.BlockSpec((STEP * BLK, 128), mine)
    return pl.pallas_call(
        call,
        grid_spec=pltpu.PrefetchScalarGridSpec(
            num_scalar_prefetch=1,
            grid=(steps,),
            in_specs=[hbm, hbm, table, gates, hbm] if final else [hbm, table, gates],
            out_specs=pl.BlockSpec((STEP * BLK, width), mine),
            scratch_shapes=[
                pltpu.VMEM((num_experts, slot_groups + WIN // GRP, GRP, width), jnp.bfloat16),
                pltpu.SemaphoreType.DMA((num_experts, slot_groups // UNIT)),
            ],
        ),
        out_shape=jax.ShapeDtypeStruct((tok, width), jnp.bfloat16),
        input_output_aliases={5: 0} if final else {},
        compiler_params=pltpu.CompilerParams(vmem_limit_bytes=56 * 2**20),
        cost_estimate=pl.CostEstimate(flops=2 * tok * num_experts * WIN * width, bytes_accessed=5 * tok * width, transcendentals=0),
        name="combine_final" if final else "combine",
    )(*((meta, back, tail, code, probs, out) if final else (meta, back, code, probs)))


def solution(mesh):
    num_experts = mesh.shape["ep_b"] * mesh.shape["ep_a"]
    tok_spec = P(("dp",) + EXPERT_AXES)
    expert_spec = P(EXPERT_AXES)

    def device_step(tokens, expert_ids, route_order, w_route, expert_keys, tau, w_in, b_in, w_out, b_out):
        tok_rows, id_row = tokens[0], expert_ids[0]
        tok, width = tok_rows.shape
        capacity = (5 * tok + 4 * num_experts - 1) // (4 * num_experts)
        slot_groups = -(-capacity // (GRP * UNIT * CHUNKS)) * UNIT * CHUNKS
        code, meta = route(route_order[0], id_row, num_experts, capacity)
        first = dispatch_first(tok_rows, code, meta, num_experts)
        send = dispatch(tok_rows, code, meta, first, slot_groups)
        first = lax.all_to_all(first, EXPERT_AXES, 0, 0, tiled=True)
        back, _, _, tail, probs = exchange(first, send, w_in[0], b_in[0], w_out[0], b_out[0], tok_rows, w_route, expert_keys, tau)
        tail = lax.all_to_all(tail, EXPERT_AXES, 0, 0, tiled=True)
        out = combine(back, None, code, meta, probs)
        return combine(back, tail, code, meta, probs, out)[None]

    return jax.shard_map(
        device_step,
        mesh=mesh,
        in_specs=(tok_spec, tok_spec, tok_spec, P(), P(), P(), expert_spec, expert_spec, expert_spec, expert_spec),
        out_specs=tok_spec,
        check_vma=False,
    )
```

```python
import functools

import jax
import jax.numpy as jnp
from jax import lax
from jax.experimental import pallas as pl
from jax.experimental.pallas import tpu as pltpu
from jax.sharding import PartitionSpec as P

EXPERT_AXES = ("ep_b", "ep_a")
CHUNKS = 5
BLK = 256
STEP = 4
GRP = 16
UNIT = 8
WIN = 64
MESH = pl.DeviceIdType.MESH
HID_TILE = 512


def onehot(mask):
    return jnp.where(mask, 1.0, 0.0)


def most(meta_ref, b, num_experts):
    n = meta_ref[1, b * num_experts]
    for e in range(1, num_experts):
        n = jnp.maximum(n, meta_ref[1, b * num_experts + e])
    return n


def place(num_experts, meta_ref, b, code, x, acc):
    span = WIN // GRP
    width = x.shape[1]
    rows = lax.broadcasted_iota(jnp.int32, (num_experts * WIN, BLK), 0)
    sub = lax.broadcasted_iota(jnp.int32, (GRP, width), 0)

    def one_pass(p, carry):
        sel = onehot(rows == code - p * (num_experts * WIN)).astype(jnp.bfloat16)
        win = jnp.dot(sel, x, preferred_element_type=jnp.float32).astype(jnp.bfloat16)
        win = win.reshape(num_experts, span, GRP, width)
        for e in range(num_experts):
            at = jnp.minimum(meta_ref[0, b * num_experts + e] + p * span, acc.shape[1] - span)
            old = jnp.where(p == 0, meta_ref[3, b * num_experts + e], 0)
            acc[e, at] = jnp.where(sub < old, acc[e, at], win[e, 0])
            acc[e, pl.ds(at + 1, span - 1)] = win[e, 1:]
        return carry

    lax.fori_loop(0, most(meta_ref, b, num_experts), one_pass, 0)


def route_kernel(num_experts, capacity, order_ref, ids_ref, grid_ref, x_ref, code_ref, meta_ref, o_ref, hot, keep, meta, slots, ring, sem_x, sem_o):
    depth = ring.shape[0]

    def load(b):
        return pltpu.make_async_copy(x_ref.at[pl.ds(pl.multiple_of(b * BLK, BLK), BLK)], ring.at[b % depth], sem_x.at[b % depth])

    for b in range(depth):
        load(b).start()
    tok = order_ref.shape[1]
    blocks = tok // BLK
    rows = blocks * num_experts
    expert_col = lax.broadcasted_iota(jnp.int32, (num_experts, BLK), 0)
    lane = lax.broadcasted_iota(jnp.int32, (BLK, BLK), 1)
    sub = lax.broadcasted_iota(jnp.int32, (BLK, BLK), 0)
    before = onehot(sub < lane).astype(jnp.bfloat16)
    ri = lax.broadcasted_iota(jnp.int32, (rows, rows), 0)
    ci = lax.broadcasted_iota(jnp.int32, (rows, rows), 1)
    same_e = (ri % num_experts) == (ci % num_experts)
    earlier_block = onehot(same_e & (ci < ri)).astype(jnp.bfloat16)
    any_block = onehot(same_e).astype(jnp.bfloat16)
    hi_iota = lax.broadcasted_iota(jnp.int32, (tok // 128, BLK), 0)
    lo_iota = lax.broadcasted_iota(jnp.int32, (128, BLK), 0)

    def hi_lo(b):
        order = order_ref[:, b * BLK:(b + 1) * BLK]
        return onehot(hi_iota == (order >> 7)).astype(jnp.bfloat16), onehot(lo_iota == (order & 127))

    def counts(oh):
        count = jnp.sum(oh, axis=1, keepdims=True)
        wide = jnp.broadcast_to(count, (rows, 128)).astype(jnp.bfloat16)
        prior = jnp.dot(earlier_block, wide, preferred_element_type=jnp.float32)
        within = jnp.dot(oh.astype(jnp.bfloat16), before, preferred_element_type=jnp.float32)
        return count, wide, prior, within

    table = jnp.transpose(grid_ref[...].astype(jnp.float32)).astype(jnp.bfloat16)
    for b in range(blocks):
        hi, lo = hi_lo(b)
        picked = jnp.dot(table, hi, preferred_element_type=jnp.float32)
        ranked = jnp.sum(picked * lo, axis=0, keepdims=True).astype(jnp.int32)
        hot[b * num_experts:(b + 1) * num_experts, :] = onehot(expert_col == ranked)
    oh = hot[...]
    _, _, prior, within = counts(oh)
    hot[...] = oh * onehot(within + prior[:, :1] < capacity)
    acc = jnp.zeros((tok // 128, 128), jnp.float32)
    for b in range(blocks):
        hi, lo = hi_lo(b)
        kept = jnp.sum(hot[b * num_experts:(b + 1) * num_experts, :], axis=0, keepdims=True)
        acc += lax.dot_general(hi * kept.astype(jnp.bfloat16), lo.astype(jnp.bfloat16), (((1,), (1,)), ((), ())), preferred_element_type=jnp.float32)
    keep[...] = acc
    for b in range(blocks):
        kept = jnp.concatenate([keep[2 * b:2 * b + 1, :], keep[2 * b + 1:2 * b + 2, :]], axis=1)
        ids = ids_ref[:, b * BLK:(b + 1) * BLK]
        hot[b * num_experts:(b + 1) * num_experts, :] = onehot(expert_col == ids) * onehot(kept > 0.5)
    oh = hot[...]
    count, wide, prior, within = counts(oh)
    total = jnp.dot(any_block, wide, preferred_element_type=jnp.float32)
    start = prior.astype(jnp.int32)
    base = start // GRP
    local = (start - base * GRP)[:, :1]
    within = within.astype(jnp.int32) + local
    expert_row = lax.broadcasted_iota(jnp.int32, (rows, BLK), 0) % num_experts
    code = (within // WIN) * (num_experts * WIN) + expert_row * WIN + within % WIN
    hot[...] = oh * (code + 1).astype(jnp.float32)
    for b in range(blocks):
        one = jnp.sum(hot[b * num_experts:(b + 1) * num_experts, :], axis=0, keepdims=True)
        code_ref[b:b + 1, :] = one.astype(jnp.int32) - 1
    need = jnp.where(count > 0.5, (local + count.astype(jnp.int32) + (WIN - 1)) // WIN, 0)
    early = jnp.zeros((1, 1), jnp.float32)
    ahead = onehot(start[:, :1] <= (capacity - UNIT * GRP) // (UNIT * GRP) * (UNIT * GRP))
    for b in range(STEP, blocks, STEP):
        early += jnp.min(ahead[b * num_experts:(b + 1) * num_experts], axis=0, keepdims=True)
    fill = jnp.ones((1, 1), jnp.float32)
    behind = onehot(start[:, :1] < UNIT * GRP)
    for b in range(1, blocks):
        fill += jnp.max(behind[b * num_experts:(b + 1) * num_experts], axis=0, keepdims=True)
    meta_ref[7:8, :] = jnp.zeros((1, rows), jnp.int32)
    meta_ref[6:7, :] = jnp.broadcast_to(fill, (1, rows)).astype(jnp.int32)
    meta_ref[5:6, :] = jnp.broadcast_to(early, (1, rows)).astype(jnp.int32)
    for row, value in enumerate((base, need, total, local, local + count.astype(jnp.int32))):
        wide = jnp.broadcast_to(value[:, :1], (rows, 128)).astype(jnp.float32)
        meta_ref[row:row + 1, :] = jnp.transpose(wide)[:1].astype(jnp.int32)
    share = pltpu.make_async_copy(meta_ref, meta, sem_o.at[0])
    share.start()
    share.wait()
    needed = meta[6, 0]

    def block(b, carry):
        load(b).wait()
        place(num_experts, meta, b, code_ref[pl.ds(b, 1), :], ring[b % depth], slots)

        @pl.when(b + depth < needed)
        def _():
            load(b + depth).start()

        return carry

    lax.fori_loop(0, needed, block, 0)
    for b in range(depth):
        @pl.when(b >= needed)
        def _():
            load(b).wait()
    outs = [pltpu.make_async_copy(slots.at[e, pl.ds(0, UNIT)], o_ref.at[e], sem_o.at[e]) for e in range(num_experts)]
    for out in outs:
        out.start()
    for out in outs:
        out.wait()


def route(order_row, id_row, tok_rows, num_experts, capacity):
    tok, width = tok_rows.shape
    blocks = tok // BLK
    rows = blocks * num_experts
    depth = min(8, blocks)
    hbm = pl.BlockSpec(memory_space=pl.ANY)
    return pl.pallas_call(
        functools.partial(route_kernel, num_experts, capacity),
        in_specs=[pl.BlockSpec(), pl.BlockSpec(), pl.BlockSpec(), hbm],
        out_specs=(pl.BlockSpec(), pl.BlockSpec(), hbm),
        out_shape=(
            jax.ShapeDtypeStruct((blocks, BLK), jnp.int32),
            jax.ShapeDtypeStruct((8, rows), jnp.int32),
            jax.ShapeDtypeStruct((num_experts, UNIT, GRP, width), jnp.bfloat16),
        ),
        scratch_shapes=[
            pltpu.VMEM((rows, BLK), jnp.float32),
            pltpu.VMEM((tok // 128, 128), jnp.float32),
            pltpu.SMEM((8, rows), jnp.int32),
            pltpu.VMEM((num_experts, UNIT + WIN // GRP, GRP, width), jnp.bfloat16),
            pltpu.VMEM((depth, BLK, width), jnp.bfloat16),
            pltpu.SemaphoreType.DMA((depth,)),
            pltpu.SemaphoreType.DMA((num_experts,)),
        ],
        compiler_params=pltpu.CompilerParams(vmem_limit_bytes=63 * 2**20),
        name="route",
    )(order_row[None], id_row[None], id_row.reshape(tok // 128, 128), tok_rows)


def used_units(meta_ref, e):
    return (meta_ref[2, e] + (UNIT * GRP - 1)) // (UNIT * GRP)


def dispatch_kernel(num_experts, meta_ref, x_ref, code_ref, _, o_ref, acc, sem):
    i, last = pl.program_id(0), pl.num_programs(0) - 1

    def block(k, carry):
        b = i * STEP + k
        x = x_ref[pl.ds(pl.multiple_of(k * BLK, BLK), BLK), :]
        place(num_experts, meta_ref, b, code_ref[pl.ds(b, 1), :], x, acc)
        return carry

    lax.fori_loop(0, STEP, block, 0)

    def unit(e, u):
        part = pl.ds(u * UNIT, UNIT)
        return pltpu.make_async_copy(acc.at[e, part], o_ref.at[e, part], sem.at[e, u])

    here, nxt = i * STEP, jnp.minimum(i + 1, last) * STEP
    for e in range(num_experts):
        begin = jnp.maximum(meta_ref[0, here * num_experts + e] // UNIT, 1)
        done = jnp.where(i == last, used_units(meta_ref, e), meta_ref[0, nxt * num_experts + e] // UNIT)
        lax.fori_loop(begin, done, lambda u, c, e=e: (unit(e, u).start(), c)[1], 0)

    @pl.when(i == last)
    def _():
        for e in range(num_experts):
            lax.fori_loop(1, used_units(meta_ref, e), lambda u, c, e=e: (unit(e, u).wait(), c)[1], 0)


def dispatch(tok_rows, code, meta, first, slot_groups):
    tok, width = tok_rows.shape
    num_experts = first.shape[0]
    padded = slot_groups + WIN // GRP
    return pl.pallas_call(
        functools.partial(dispatch_kernel, num_experts),
        grid_spec=pltpu.PrefetchScalarGridSpec(
            num_scalar_prefetch=1,
            grid=(tok // (BLK * STEP),),
            in_specs=[
                pl.BlockSpec((STEP * BLK, width), lambda i, *_: (i, 0)),
                pl.BlockSpec(code.shape, lambda i, *_: (0, 0)),
                pl.BlockSpec(memory_space=pl.ANY),
            ],
            out_specs=pl.BlockSpec(memory_space=pl.ANY),
            scratch_shapes=[
                pltpu.VMEM((num_experts, padded, GRP, width), jnp.bfloat16),
                pltpu.SemaphoreType.DMA((num_experts, slot_groups // UNIT)),
            ],
        ),
        out_shape=jax.ShapeDtypeStruct((num_experts, slot_groups, GRP, width), jnp.bfloat16),
        compiler_params=pltpu.CompilerParams(vmem_limit_bytes=63 * 2**20),
        cost_estimate=pl.CostEstimate(flops=2 * tok * num_experts * WIN * width, bytes_accessed=5 * tok * width, transcendentals=0),
        name="dispatch",
    )(meta, tok_rows, code, first)


def partner(d):
    row, col = lax.axis_index("ep_b"), lax.axis_index("ep_a")
    to_row = (row + d // 4) % 2
    to_col = ((col // 2 + (d // 2) % 2) % 2) * 2 + (col % 2 + d % 2) % 2
    return to_row * 4 + to_col, {"ep_b": to_row, "ep_a": to_col}


def exchange_kernel(num_experts, slot_groups, first, send, w1_hbm, b1_ref, w2_hbm, b2_ref, tokens, wr_ref, keys_ref, tau_ref, back, recv, staged, tail, probs, w1, w2, x, y, h, prob, sem_w, sem_x, sem_y, out_s, out_r, ret_s, ret_r):
    cg = slot_groups // CHUNKS
    units = slot_groups // UNIT
    me, _ = partner(0)

    def to_expert(d, u):
        peer, where = partner(d)
        part = pl.ds(u * UNIT, UNIT)
        return pltpu.make_async_remote_copy(send.at[peer, part], recv.at[d, part], out_s.at[d, u], out_r.at[d, u], device_id=where, device_id_type=MESH)

    def to_owner(d, u):
        _, where = partner(d)
        part = pl.ds(u * UNIT, UNIT)
        return pltpu.make_async_remote_copy(staged.at[d, part], back.at[me, part], ret_s.at[d, u], ret_r.at[d, u], device_id=where, device_id_type=MESH)

    barrier = pltpu.get_barrier_semaphore()
    for d in range(1, num_experts):
        pl.semaphore_signal(barrier, inc=1, device_id=partner(d)[1], device_id_type=MESH)
    pl.semaphore_wait(barrier, num_experts - 1)

    far_first = (6, 4, 2, 7, 5, 3, 1)
    for u in range(1, units):
        for d in far_first:
            to_expert(d, u).start()
    load1 = pltpu.make_async_copy(w1_hbm, w1, sem_w.at[0])
    load2 = pltpu.make_async_copy(w2_hbm, w2, sem_w.at[1])
    load1.start()
    load2.start()
    load1.wait()
    load2.wait()

    def step(i, carry):
        c, g = i // (num_experts // 2), i % (num_experts // 2)
        per = cg // UNIT

        def take(src, half, k):
            return pltpu.make_async_copy(src, x.at[half, pl.ds(k * UNIT, UNIT)], sem_x.at[half, k])

        for half in range(2):
            d = 2 * g + half
            for k in range(per):
                u = c * per + k
                part = pl.ds(u * UNIT, UNIT)

                @pl.when(u == 0)
                def _():
                    take(first.at[partner(d)[0]], half, k).start()

                @pl.when((u != 0) & (d == 0))
                def _():
                    take(send.at[me, part], half, k).start()

                @pl.when((u != 0) & (d != 0))
                def _():
                    to_expert(d, u).wait_recv()
                    take(recv.at[d, part], half, k).start()
        for half in range(2):
            for k in range(per):
                take(first.at[me], half, k).wait()

        rows = x[...].reshape(2 * cg * GRP, x.shape[3])
        for j in range(w1.shape[1] // HID_TILE):
            cols = pl.ds(j * HID_TILE, HID_TILE)
            pre = jnp.dot(rows, w1[:, cols], preferred_element_type=jnp.float32) + b1_ref[:, cols].astype(jnp.float32)
            act = pre * 0.5 * (1.0 + lax.erf(pre * 0.7071067811865476))
            h[:, cols] = act.astype(jnp.bfloat16)
        hidden = h[...]
        for j in range(w2.shape[1] // 256):
            cols = pl.ds(j * 256, 256)
            res = jnp.dot(hidden, w2[:, cols], preferred_element_type=jnp.float32) + b2_ref[:, cols].astype(jnp.float32)
            y[:, :, :, cols] = res.astype(jnp.bfloat16).reshape(2, cg, GRP, 256)

        def put(half, k, dst):
            return pltpu.make_async_copy(y.at[half, pl.ds(k * UNIT, UNIT)], dst, sem_y.at[half, k])

        for half in range(2):
            d = 2 * g + half
            for k in range(per):
                u = c * per + k
                part = pl.ds(u * UNIT, UNIT)

                @pl.when(u == units - 1)
                def _():
                    put(half, k, tail.at[partner(d)[0]]).start()

                @pl.when((u != units - 1) & (d == 0))
                def _():
                    put(half, k, back.at[me, part]).start()

                @pl.when((u != units - 1) & (d != 0))
                def _():
                    put(half, k, staged.at[d, part]).start()

        for half in range(2):
            d = 2 * g + half
            for k in range(per):
                u = c * per + k
                put(half, k, tail.at[me]).wait()

                @pl.when((u != units - 1) & (d != 0))
                def _():
                    to_owner(d, u).start()
        return carry

    lax.fori_loop(0, CHUNKS * num_experts // 2, step, 0)

    keys = keys_ref[...].astype(jnp.float32)
    unit_keys = keys / jnp.sqrt(jnp.sum(keys * keys, axis=1, keepdims=True))
    unit_keys = jnp.concatenate([unit_keys, jnp.zeros((128 - num_experts, keys.shape[1]), jnp.float32)], axis=0)
    real = lax.broadcasted_iota(jnp.int32, prob.shape, 1) < num_experts

    def gate_step(i, carry):
        for half in range(2):
            got = pltpu.make_async_copy(tokens.at[pl.ds((2 * i + half) * cg, cg)], x.at[half], sem_x.at[half, 0])
            got.start()
            got.wait()
        proj = jnp.dot(x[...].reshape(prob.shape[0], x.shape[3]), wr_ref[...], preferred_element_type=jnp.float32)
        unit = proj / jnp.sqrt(jnp.sum(proj * proj, axis=1, keepdims=True))
        logits = lax.dot_general(unit, unit_keys, (((1,), (1,)), ((), ())), preferred_element_type=jnp.float32) / tau_ref[0, 0]
        top = jnp.max(jnp.where(real, logits, -jnp.inf), axis=1, keepdims=True)
        weight = jnp.where(real, jnp.exp(logits - top), 0.0)
        prob[...] = weight / jnp.sum(weight, axis=1, keepdims=True)
        put = pltpu.make_async_copy(prob, probs.at[pl.ds(i * prob.shape[0], prob.shape[0])], sem_y.at[0, 0])
        put.start()
        put.wait()
        return carry

    lax.fori_loop(0, probs.shape[0] // prob.shape[0], gate_step, 0)
    for u in range(1, units):
        for d in range(1, num_experts):
            to_expert(d, u).wait_send()
    for u in range(units - 1):
        for d in range(1, num_experts):
            to_owner(d, u).wait()


def exchange(first, send, w_first, b_first, w_second, b_second, tok_rows, w_route, expert_keys, tau):
    num_experts, slot_groups, _, width = send.shape
    tok = tok_rows.shape[0]
    hidden = w_first.shape[1]
    cg = slot_groups // CHUNKS
    land = jax.ShapeDtypeStruct((num_experts, slot_groups, GRP, width), jnp.bfloat16)
    tail = jax.ShapeDtypeStruct((num_experts, UNIT, GRP, width), jnp.bfloat16)
    probs = jax.ShapeDtypeStruct((tok, 128), jnp.float32)
    sems = pltpu.SemaphoreType.DMA((num_experts, slot_groups // UNIT))
    hbm = pl.BlockSpec(memory_space=pl.ANY)
    vmem = pl.BlockSpec(memory_space=pltpu.VMEM)
    return pl.pallas_call(
        functools.partial(exchange_kernel, num_experts, slot_groups),
        out_shape=(land, land, land, tail, probs),
        in_specs=[hbm, hbm, hbm, vmem, hbm, vmem, hbm, vmem, vmem, pl.BlockSpec(memory_space=pltpu.SMEM)],
        out_specs=(hbm, hbm, hbm, hbm, hbm),
        scratch_shapes=[
            pltpu.VMEM((width, hidden), jnp.bfloat16),
            pltpu.VMEM((hidden, width), jnp.bfloat16),
            pltpu.VMEM((2, cg, GRP, width), jnp.bfloat16),
            pltpu.VMEM((2, cg, GRP, width), jnp.bfloat16),
            pltpu.VMEM((2 * cg * GRP, hidden), jnp.bfloat16),
            pltpu.VMEM((2 * cg * GRP, 128), jnp.float32),
            pltpu.SemaphoreType.DMA((2,)),
            pltpu.SemaphoreType.DMA((2, cg // UNIT)),
            pltpu.SemaphoreType.DMA((2, cg // UNIT)),
            sems, sems, sems, sems,
        ],
        compiler_params=pltpu.CompilerParams(collective_id=0, has_side_effects=True, vmem_limit_bytes=60 * 2**20),
        name="exchange",
    )(first, send, w_first, b_first[None], w_second, b_second[None], tok_rows.reshape(tok // GRP, GRP, width), w_route, expert_keys, tau.reshape(1, 1))


def combine_kernel(num_experts, final, meta_ref, back_ref, tail_ref, code_ref, prob_ref, o_ref, rows_in, sem):
    early = meta_ref[5, 0]
    first = early if final else 0
    i, last = pl.program_id(0), pl.num_programs(0) - 1
    span = WIN // GRP
    width = o_ref.shape[1]
    units = sem.shape[1]
    cols = lax.broadcasted_iota(jnp.int32, (BLK, 128), 1)
    row = lax.broadcasted_iota(jnp.int32, (WIN, width), 0)

    def unit(e, u, from_tail=False):
        part = pl.ds(u * UNIT, UNIT)
        return pltpu.make_async_copy(tail_ref.at[e] if from_tail else back_ref.at[e, part], rows_in.at[e, part], sem.at[e, u])

    def rows_before(step, e):
        n = step * STEP * num_experts + e
        return meta_ref[0, n] * GRP + meta_ref[3, n]

    def reach(step, e):
        return (rows_before(step, e) + (UNIT * GRP - 1)) // (UNIT * GRP)

    def block(k, carry):
        b = i * STEP + k
        mine = pl.ds(pl.multiple_of(k * BLK, BLK), BLK)
        code = jnp.transpose(jnp.broadcast_to(code_ref[pl.ds(b, 1), :], (128, BLK)))
        expert = (code & (num_experts * WIN - 1)) // WIN
        gate = jnp.sum(jnp.where(cols == expert, prob_ref[mine, :], 0.0), axis=1, keepdims=True)

        def picked(p):
            sel = jnp.concatenate([onehot(cols + k == code - p * (num_experts * WIN)) for k in range(0, num_experts * WIN, 128)], axis=1)
            wins = []
            for e in range(num_experts):
                at = jnp.minimum(meta_ref[0, b * num_experts + e] + p * span, rows_in.shape[1] - span)
                rows = rows_in[e, pl.ds(at, span)].reshape(WIN, width)
                end = meta_ref[0, b * num_experts + e] * GRP + meta_ref[4, b * num_experts + e]
                wins.append(jnp.where(row < end - at * GRP, rows, jnp.zeros_like(rows)))
            return jnp.dot(sel.astype(jnp.bfloat16), jnp.concatenate(wins, axis=0), preferred_element_type=jnp.float32)

        o_ref[mine, :] = (gate * picked(0)).astype(jnp.bfloat16)

        def more(p, carry):
            o_ref[mine, :] += (gate * picked(p)).astype(jnp.bfloat16)
            return carry

        return lax.fori_loop(1, most(meta_ref, b, num_experts), more, carry)

    @pl.when(i == first)
    def _():
        for u in range(units if final else units - 1):
            for e in range(num_experts):
                if final:
                    wanted = (u >= rows_before(early, e) // (UNIT * GRP)) & (u < used_units(meta_ref, e))
                else:
                    wanted = u < reach(early, e)

                @pl.when(wanted)
                def _():
                    unit(e, u, u == units - 1).start()

    @pl.when((i >= early) if final else (i < early))
    def _():
        for e in range(num_experts):
            begin = reach(i, e)
            end = reach(jnp.minimum(i + 1, last), e)
            if final:
                begin = jnp.where(i == early, rows_before(early, e) // (UNIT * GRP), begin)
                end = jnp.where(i == last, used_units(meta_ref, e), end)
            lax.fori_loop(begin, end, lambda u, c, e=e: (unit(e, u).wait(), c)[1], 0)
        lax.fori_loop(0, STEP, block, 0)


def combine(back, tail, code, meta, probs, out=None):
    tok, width = probs.shape[0], back.shape[3]
    num_experts, slot_groups = back.shape[:2]
    final = out is not None
    steps = tok // (BLK * STEP)
    kernel = functools.partial(combine_kernel, num_experts, final)
    hbm = pl.BlockSpec(memory_space=pl.ANY)

    def mine(i, meta_ref):
        return (jnp.maximum(i, meta_ref[5, 0]), 0) if final else (jnp.minimum(i, jnp.maximum(meta_ref[5, 0] - 1, 0)), 0)

    def call(meta_ref, *refs):
        if final:
            back_ref, tail_ref, code_ref, prob_ref, _, *rest = refs
        else:
            back_ref, code_ref, prob_ref, *rest = refs
            tail_ref = None
        kernel(meta_ref, back_ref, tail_ref, code_ref, prob_ref, *rest)

    table = pl.BlockSpec(code.shape, lambda i, *_: (0, 0))
    gates = pl.BlockSpec((STEP * BLK, 128), mine)
    return pl.pallas_call(
        call,
        grid_spec=pltpu.PrefetchScalarGridSpec(
            num_scalar_prefetch=1,
            grid=(steps,),
            in_specs=[hbm, hbm, table, gates, hbm] if final else [hbm, table, gates],
            out_specs=pl.BlockSpec((STEP * BLK, width), mine),
            scratch_shapes=[
                pltpu.VMEM((num_experts, slot_groups + WIN // GRP, GRP, width), jnp.bfloat16),
                pltpu.SemaphoreType.DMA((num_experts, slot_groups // UNIT)),
            ],
        ),
        out_shape=jax.ShapeDtypeStruct((tok, width), jnp.bfloat16),
        input_output_aliases={5: 0} if final else {},
        compiler_params=pltpu.CompilerParams(vmem_limit_bytes=63 * 2**20),
        cost_estimate=pl.CostEstimate(flops=2 * tok * num_experts * WIN * width, bytes_accessed=5 * tok * width, transcendentals=0),
        name="combine_final" if final else "combine",
    )(*((meta, back, tail, code, probs, out) if final else (meta, back, code, probs)))


def solution(mesh):
    num_experts = mesh.shape["ep_b"] * mesh.shape["ep_a"]
    tok_spec = P(("dp",) + EXPERT_AXES)
    expert_spec = P(EXPERT_AXES)

    def device_step(tokens, expert_ids, route_order, w_route, expert_keys, tau, w_in, b_in, w_out, b_out):
        tok_rows, id_row = tokens[0], expert_ids[0]
        tok, width = tok_rows.shape
        capacity = (5 * tok + 4 * num_experts - 1) // (4 * num_experts)
        slot_groups = -(-capacity // (GRP * UNIT * CHUNKS)) * UNIT * CHUNKS
        code, meta, first = route(route_order[0], id_row, tok_rows, num_experts, capacity)
        send = dispatch(tok_rows, code, meta, first, slot_groups)
        first = lax.all_to_all(first, EXPERT_AXES, 0, 0, tiled=True)
        back, _, _, tail, probs = exchange(first, send, w_in[0], b_in[0], w_out[0], b_out[0], tok_rows, w_route, expert_keys, tau)
        tail = lax.all_to_all(tail, EXPERT_AXES, 0, 0, tiled=True)
        out = combine(back, None, code, meta, probs)
        return combine(back, tail, code, meta, probs, out)[None]

    return jax.shard_map(
        device_step,
        mesh=mesh,
        in_specs=(tok_spec, tok_spec, tok_spec, P(), P(), P(), expert_spec, expert_spec, expert_spec, expert_spec),
        out_specs=tok_spec,
        check_vma=False,
    )
```

```python
import functools

import jax
import jax.numpy as jnp
from jax import lax
from jax.experimental import pallas as pl
from jax.experimental.pallas import tpu as pltpu
from jax.sharding import PartitionSpec as P

EXPERT_AXES = ("ep_b", "ep_a")
CHUNKS = 5
BLK = 256
STEP = 2
GRP = 16
UNIT = 8
WIN = 64
MESH = pl.DeviceIdType.MESH
HID_TILE = 512


def onehot(mask):
    return jnp.where(mask, 1.0, 0.0)


def most(meta_ref, b, num_experts):
    n = meta_ref[1, b * num_experts]
    for e in range(1, num_experts):
        n = jnp.maximum(n, meta_ref[1, b * num_experts + e])
    return n


def place(num_experts, meta_ref, b, code, x, acc):
    span = WIN // GRP
    width = x.shape[1]
    rows = lax.broadcasted_iota(jnp.int32, (num_experts * WIN, BLK), 0)
    sub = lax.broadcasted_iota(jnp.int32, (GRP, width), 0)

    def one_pass(p, carry):
        sel = onehot(rows == code - p * (num_experts * WIN)).astype(jnp.bfloat16)
        win = jnp.dot(sel, x, preferred_element_type=jnp.float32).astype(jnp.bfloat16)
        win = win.reshape(num_experts, span, GRP, width)
        for e in range(num_experts):
            at = jnp.minimum(meta_ref[0, b * num_experts + e] + p * span, acc.shape[1] - span)
            old = jnp.where(p == 0, meta_ref[3, b * num_experts + e], 0)
            acc[e, at] = jnp.where(sub < old, acc[e, at], win[e, 0])
            acc[e, pl.ds(at + 1, span - 1)] = win[e, 1:]
        return carry

    lax.fori_loop(0, most(meta_ref, b, num_experts), one_pass, 0)


def route_kernel(num_experts, capacity, order_ref, ids_ref, grid_ref, x_ref, code_ref, meta_ref, o_ref, hot, keep, meta, slots, ring, sem_x, sem_o):
    depth = ring.shape[0]

    def load(b):
        return pltpu.make_async_copy(x_ref.at[pl.ds(pl.multiple_of(b * BLK, BLK), BLK)], ring.at[b % depth], sem_x.at[b % depth])

    for b in range(depth):
        load(b).start()
    tok = order_ref.shape[1]
    blocks = tok // BLK
    rows = blocks * num_experts
    expert_col = lax.broadcasted_iota(jnp.int32, (num_experts, BLK), 0)
    lane = lax.broadcasted_iota(jnp.int32, (BLK, BLK), 1)
    sub = lax.broadcasted_iota(jnp.int32, (BLK, BLK), 0)
    before = onehot(sub < lane).astype(jnp.bfloat16)
    ri = lax.broadcasted_iota(jnp.int32, (rows, rows), 0)
    ci = lax.broadcasted_iota(jnp.int32, (rows, rows), 1)
    same_e = (ri % num_experts) == (ci % num_experts)
    earlier_block = onehot(same_e & (ci < ri)).astype(jnp.bfloat16)
    any_block = onehot(same_e).astype(jnp.bfloat16)
    hi_iota = lax.broadcasted_iota(jnp.int32, (tok // 128, BLK), 0)
    lo_iota = lax.broadcasted_iota(jnp.int32, (128, BLK), 0)

    def hi_lo(b):
        order = order_ref[:, b * BLK:(b + 1) * BLK]
        return onehot(hi_iota == (order >> 7)).astype(jnp.bfloat16), onehot(lo_iota == (order & 127))

    def counts(oh):
        count = jnp.sum(oh, axis=1, keepdims=True)
        wide = jnp.broadcast_to(count, (rows, 128)).astype(jnp.bfloat16)
        prior = jnp.dot(earlier_block, wide, preferred_element_type=jnp.float32)
        within = jnp.dot(oh.astype(jnp.bfloat16), before, preferred_element_type=jnp.float32)
        return count, wide, prior, within

    table = jnp.transpose(grid_ref[...].astype(jnp.float32)).astype(jnp.bfloat16)
    for b in range(blocks):
        hi, lo = hi_lo(b)
        picked = jnp.dot(table, hi, preferred_element_type=jnp.float32)
        ranked = jnp.sum(picked * lo, axis=0, keepdims=True).astype(jnp.int32)
        hot[b * num_experts:(b + 1) * num_experts, :] = onehot(expert_col == ranked)
    oh = hot[...]
    _, _, prior, within = counts(oh)
    hot[...] = oh * onehot(within + prior[:, :1] < capacity)
    acc = jnp.zeros((tok // 128, 128), jnp.float32)
    for b in range(blocks):
        hi, lo = hi_lo(b)
        kept = jnp.sum(hot[b * num_experts:(b + 1) * num_experts, :], axis=0, keepdims=True)
        acc += lax.dot_general(hi * kept.astype(jnp.bfloat16), lo.astype(jnp.bfloat16), (((1,), (1,)), ((), ())), preferred_element_type=jnp.float32)
    keep[...] = acc
    for b in range(blocks):
        kept = jnp.concatenate([keep[2 * b:2 * b + 1, :], keep[2 * b + 1:2 * b + 2, :]], axis=1)
        ids = ids_ref[:, b * BLK:(b + 1) * BLK]
        hot[b * num_experts:(b + 1) * num_experts, :] = onehot(expert_col == ids) * onehot(kept > 0.5)
    oh = hot[...]
    count, wide, prior, within = counts(oh)
    total = jnp.dot(any_block, wide, preferred_element_type=jnp.float32)
    start = prior.astype(jnp.int32)
    base = start // GRP
    local = (start - base * GRP)[:, :1]
    within = within.astype(jnp.int32) + local
    expert_row = lax.broadcasted_iota(jnp.int32, (rows, BLK), 0) % num_experts
    code = (within // WIN) * (num_experts * WIN) + expert_row * WIN + within % WIN
    hot[...] = oh * (code + 1).astype(jnp.float32)
    for b in range(blocks):
        one = jnp.sum(hot[b * num_experts:(b + 1) * num_experts, :], axis=0, keepdims=True)
        code_ref[b:b + 1, :] = one.astype(jnp.int32) - 1
    need = jnp.where(count > 0.5, (local + count.astype(jnp.int32) + (WIN - 1)) // WIN, 0)
    early = jnp.zeros((1, 1), jnp.float32)
    ahead = onehot(start[:, :1] <= (capacity - UNIT * GRP) // (UNIT * GRP) * (UNIT * GRP))
    for b in range(STEP, blocks, STEP):
        early += jnp.min(ahead[b * num_experts:(b + 1) * num_experts], axis=0, keepdims=True)
    fill = jnp.ones((1, 1), jnp.float32)
    behind = onehot(start[:, :1] < UNIT * GRP)
    for b in range(1, blocks):
        fill += jnp.max(behind[b * num_experts:(b + 1) * num_experts], axis=0, keepdims=True)
    meta_ref[7:8, :] = jnp.zeros((1, rows), jnp.int32)
    meta_ref[6:7, :] = jnp.broadcast_to(fill, (1, rows)).astype(jnp.int32)
    meta_ref[5:6, :] = jnp.broadcast_to(early, (1, rows)).astype(jnp.int32)
    for row, value in enumerate((base, need, total, local, local + count.astype(jnp.int32))):
        wide = jnp.broadcast_to(value[:, :1], (rows, 128)).astype(jnp.float32)
        meta_ref[row:row + 1, :] = jnp.transpose(wide)[:1].astype(jnp.int32)
    share = pltpu.make_async_copy(meta_ref, meta, sem_o.at[0])
    share.start()
    share.wait()
    needed = meta[6, 0]

    def block(b, carry):
        load(b).wait()
        place(num_experts, meta, b, code_ref[pl.ds(b, 1), :], ring[b % depth], slots)

        @pl.when(b + depth < needed)
        def _():
            load(b + depth).start()

        return carry

    lax.fori_loop(0, needed, block, 0)
    for b in range(depth):
        @pl.when(b >= needed)
        def _():
            load(b).wait()
    outs = [pltpu.make_async_copy(slots.at[e, pl.ds(0, UNIT)], o_ref.at[e], sem_o.at[e]) for e in range(num_experts)]
    for out in outs:
        out.start()
    for out in outs:
        out.wait()


def route(order_row, id_row, tok_rows, num_experts, capacity):
    tok, width = tok_rows.shape
    blocks = tok // BLK
    rows = blocks * num_experts
    depth = min(8, blocks)
    hbm = pl.BlockSpec(memory_space=pl.ANY)
    return pl.pallas_call(
        functools.partial(route_kernel, num_experts, capacity),
        in_specs=[pl.BlockSpec(), pl.BlockSpec(), pl.BlockSpec(), hbm],
        out_specs=(pl.BlockSpec(), pl.BlockSpec(), hbm),
        out_shape=(
            jax.ShapeDtypeStruct((blocks, BLK), jnp.int32),
            jax.ShapeDtypeStruct((8, rows), jnp.int32),
            jax.ShapeDtypeStruct((num_experts, UNIT, GRP, width), jnp.bfloat16),
        ),
        scratch_shapes=[
            pltpu.VMEM((rows, BLK), jnp.float32),
            pltpu.VMEM((tok // 128, 128), jnp.float32),
            pltpu.SMEM((8, rows), jnp.int32),
            pltpu.VMEM((num_experts, UNIT + WIN // GRP, GRP, width), jnp.bfloat16),
            pltpu.VMEM((depth, BLK, width), jnp.bfloat16),
            pltpu.SemaphoreType.DMA((depth,)),
            pltpu.SemaphoreType.DMA((num_experts,)),
        ],
        compiler_params=pltpu.CompilerParams(vmem_limit_bytes=63 * 2**20),
        name="route",
    )(order_row[None], id_row[None], id_row.reshape(tok // 128, 128), tok_rows)


def used_units(meta_ref, e):
    return (meta_ref[2, e] + (UNIT * GRP - 1)) // (UNIT * GRP)


def dispatch_kernel(num_experts, meta_ref, x_ref, code_ref, _, o_ref, acc, sem):
    i, last = pl.program_id(0), pl.num_programs(0) - 1

    def block(k, carry):
        b = i * STEP + k
        x = x_ref[pl.ds(pl.multiple_of(k * BLK, BLK), BLK), :]
        place(num_experts, meta_ref, b, code_ref[pl.ds(b, 1), :], x, acc)
        return carry

    lax.fori_loop(0, STEP, block, 0)

    def unit(e, u):
        part = pl.ds(u * UNIT, UNIT)
        return pltpu.make_async_copy(acc.at[e, part], o_ref.at[e, part], sem.at[e, u])

    here, nxt = i * STEP, jnp.minimum(i + 1, last) * STEP
    for e in range(num_experts):
        begin = jnp.maximum(meta_ref[0, here * num_experts + e] // UNIT, 1)
        done = jnp.where(i == last, used_units(meta_ref, e), meta_ref[0, nxt * num_experts + e] // UNIT)
        lax.fori_loop(begin, done, lambda u, c, e=e: (unit(e, u).start(), c)[1], 0)

    @pl.when(i == last)
    def _():
        for e in range(num_experts):
            lax.fori_loop(1, used_units(meta_ref, e), lambda u, c, e=e: (unit(e, u).wait(), c)[1], 0)


def dispatch(tok_rows, code, meta, first, slot_groups):
    tok, width = tok_rows.shape
    num_experts = first.shape[0]
    padded = slot_groups + WIN // GRP
    return pl.pallas_call(
        functools.partial(dispatch_kernel, num_experts),
        grid_spec=pltpu.PrefetchScalarGridSpec(
            num_scalar_prefetch=1,
            grid=(tok // (BLK * STEP),),
            in_specs=[
                pl.BlockSpec((STEP * BLK, width), lambda i, *_: (i, 0)),
                pl.BlockSpec(code.shape, lambda i, *_: (0, 0)),
                pl.BlockSpec(memory_space=pl.ANY),
            ],
            out_specs=pl.BlockSpec(memory_space=pl.ANY),
            scratch_shapes=[
                pltpu.VMEM((num_experts, padded, GRP, width), jnp.bfloat16),
                pltpu.SemaphoreType.DMA((num_experts, slot_groups // UNIT)),
            ],
        ),
        out_shape=jax.ShapeDtypeStruct((num_experts, slot_groups, GRP, width), jnp.bfloat16),
        compiler_params=pltpu.CompilerParams(vmem_limit_bytes=63 * 2**20),
        cost_estimate=pl.CostEstimate(flops=2 * tok * num_experts * WIN * width, bytes_accessed=5 * tok * width, transcendentals=0),
        name="dispatch",
    )(meta, tok_rows, code, first)


def partner(d):
    row, col = lax.axis_index("ep_b"), lax.axis_index("ep_a")
    to_row = (row + d // 4) % 2
    to_col = ((col // 2 + (d // 2) % 2) % 2) * 2 + (col % 2 + d % 2) % 2
    return to_row * 4 + to_col, {"ep_b": to_row, "ep_a": to_col}


def exchange_kernel(num_experts, slot_groups, first, send, w1_hbm, b1_ref, w2_hbm, b2_ref, tokens, wr_ref, keys_ref, tau_ref, back, recv, staged, tail, probs, w1, w2, x, y, h, prob, sem_w, sem_x, sem_y, out_s, out_r, ret_s, ret_r):
    cg = slot_groups // CHUNKS
    units = slot_groups // UNIT
    me, _ = partner(0)

    def to_expert(d, u):
        peer, where = partner(d)
        part = pl.ds(u * UNIT, UNIT)
        return pltpu.make_async_remote_copy(send.at[peer, part], recv.at[d, part], out_s.at[d, u], out_r.at[d, u], device_id=where, device_id_type=MESH)

    def to_owner(d, u):
        _, where = partner(d)
        part = pl.ds(u * UNIT, UNIT)
        return pltpu.make_async_remote_copy(staged.at[d, part], back.at[me, part], ret_s.at[d, u], ret_r.at[d, u], device_id=where, device_id_type=MESH)

    barrier = pltpu.get_barrier_semaphore()
    for d in range(1, num_experts):
        pl.semaphore_signal(barrier, inc=1, device_id=partner(d)[1], device_id_type=MESH)
    pl.semaphore_wait(barrier, num_experts - 1)

    far_first = (6, 4, 2, 7, 5, 3, 1)
    for u in range(1, units):
        for d in far_first:
            to_expert(d, u).start()
    load1 = pltpu.make_async_copy(w1_hbm, w1, sem_w.at[0])
    load2 = pltpu.make_async_copy(w2_hbm, w2, sem_w.at[1])
    load1.start()
    load2.start()
    load1.wait()
    load2.wait()

    def step(i, carry):
        c, g = i // (num_experts // 2), i % (num_experts // 2)
        per = cg // UNIT

        def take(src, half, k):
            return pltpu.make_async_copy(src, x.at[half, pl.ds(k * UNIT, UNIT)], sem_x.at[half, k])

        for half in range(2):
            d = 2 * g + half
            for k in range(per):
                u = c * per + k
                part = pl.ds(u * UNIT, UNIT)

                @pl.when(u == 0)
                def _():
                    take(first.at[partner(d)[0]], half, k).start()

                @pl.when((u != 0) & (d == 0))
                def _():
                    take(send.at[me, part], half, k).start()

                @pl.when((u != 0) & (d != 0))
                def _():
                    to_expert(d, u).wait_recv()
                    take(recv.at[d, part], half, k).start()
        for half in range(2):
            for k in range(per):
                take(first.at[me], half, k).wait()

        rows = x[...].reshape(2 * cg * GRP, x.shape[3])
        for j in range(w1.shape[1] // HID_TILE):
            cols = pl.ds(j * HID_TILE, HID_TILE)
            pre = jnp.dot(rows, w1[:, cols], preferred_element_type=jnp.float32) + b1_ref[:, cols].astype(jnp.float32)
            act = pre * 0.5 * (1.0 + lax.erf(pre * 0.7071067811865476))
            h[:, cols] = act.astype(jnp.bfloat16)
        hidden = h[...]
        for j in range(w2.shape[1] // 256):
            cols = pl.ds(j * 256, 256)
            res = jnp.dot(hidden, w2[:, cols], preferred_element_type=jnp.float32) + b2_ref[:, cols].astype(jnp.float32)
            y[:, :, :, cols] = res.astype(jnp.bfloat16).reshape(2, cg, GRP, 256)

        def put(half, k, dst):
            return pltpu.make_async_copy(y.at[half, pl.ds(k * UNIT, UNIT)], dst, sem_y.at[half, k])

        for half in range(2):
            d = 2 * g + half
            for k in range(per):
                u = c * per + k
                part = pl.ds(u * UNIT, UNIT)

                @pl.when(u == units - 1)
                def _():
                    put(half, k, tail.at[partner(d)[0]]).start()

                @pl.when((u != units - 1) & (d == 0))
                def _():
                    put(half, k, back.at[me, part]).start()

                @pl.when((u != units - 1) & (d != 0))
                def _():
                    put(half, k, staged.at[d, part]).start()

        for half in range(2):
            d = 2 * g + half
            for k in range(per):
                u = c * per + k
                put(half, k, tail.at[me]).wait()

                @pl.when((u != units - 1) & (d != 0))
                def _():
                    to_owner(d, u).start()
        return carry

    lax.fori_loop(0, CHUNKS * num_experts // 2, step, 0)

    keys = keys_ref[...].astype(jnp.float32)
    unit_keys = keys / jnp.sqrt(jnp.sum(keys * keys, axis=1, keepdims=True))
    unit_keys = jnp.concatenate([unit_keys, jnp.zeros((128 - num_experts, keys.shape[1]), jnp.float32)], axis=0)
    real = lax.broadcasted_iota(jnp.int32, prob.shape, 1) < num_experts

    def gate_step(i, carry):
        for half in range(2):
            got = pltpu.make_async_copy(tokens.at[pl.ds((2 * i + half) * cg, cg)], x.at[half], sem_x.at[half, 0])
            got.start()
            got.wait()
        proj = jnp.dot(x[...].reshape(prob.shape[0], x.shape[3]), wr_ref[...], preferred_element_type=jnp.float32)
        unit = proj / jnp.sqrt(jnp.sum(proj * proj, axis=1, keepdims=True))
        logits = lax.dot_general(unit, unit_keys, (((1,), (1,)), ((), ())), preferred_element_type=jnp.float32) / tau_ref[0, 0]
        top = jnp.max(jnp.where(real, logits, -jnp.inf), axis=1, keepdims=True)
        weight = jnp.where(real, jnp.exp(logits - top), 0.0)
        prob[...] = weight / jnp.sum(weight, axis=1, keepdims=True)
        put = pltpu.make_async_copy(prob, probs.at[pl.ds(i * prob.shape[0], prob.shape[0])], sem_y.at[0, 0])
        put.start()
        put.wait()
        return carry

    lax.fori_loop(0, probs.shape[0] // prob.shape[0], gate_step, 0)
    for u in range(1, units):
        for d in range(1, num_experts):
            to_expert(d, u).wait_send()
    for u in range(units - 1):
        for d in range(1, num_experts):
            to_owner(d, u).wait()


def exchange(first, send, w_first, b_first, w_second, b_second, tok_rows, w_route, expert_keys, tau):
    num_experts, slot_groups, _, width = send.shape
    tok = tok_rows.shape[0]
    hidden = w_first.shape[1]
    cg = slot_groups // CHUNKS
    land = jax.ShapeDtypeStruct((num_experts, slot_groups, GRP, width), jnp.bfloat16)
    tail = jax.ShapeDtypeStruct((num_experts, UNIT, GRP, width), jnp.bfloat16)
    probs = jax.ShapeDtypeStruct((tok, 128), jnp.float32)
    sems = pltpu.SemaphoreType.DMA((num_experts, slot_groups // UNIT))
    hbm = pl.BlockSpec(memory_space=pl.ANY)
    vmem = pl.BlockSpec(memory_space=pltpu.VMEM)
    return pl.pallas_call(
        functools.partial(exchange_kernel, num_experts, slot_groups),
        out_shape=(land, land, land, tail, probs),
        in_specs=[hbm, hbm, hbm, vmem, hbm, vmem, hbm, vmem, vmem, pl.BlockSpec(memory_space=pltpu.SMEM)],
        out_specs=(hbm, hbm, hbm, hbm, hbm),
        scratch_shapes=[
            pltpu.VMEM((width, hidden), jnp.bfloat16),
            pltpu.VMEM((hidden, width), jnp.bfloat16),
            pltpu.VMEM((2, cg, GRP, width), jnp.bfloat16),
            pltpu.VMEM((2, cg, GRP, width), jnp.bfloat16),
            pltpu.VMEM((2 * cg * GRP, hidden), jnp.bfloat16),
            pltpu.VMEM((2 * cg * GRP, 128), jnp.float32),
            pltpu.SemaphoreType.DMA((2,)),
            pltpu.SemaphoreType.DMA((2, cg // UNIT)),
            pltpu.SemaphoreType.DMA((2, cg // UNIT)),
            sems, sems, sems, sems,
        ],
        compiler_params=pltpu.CompilerParams(collective_id=0, has_side_effects=True, vmem_limit_bytes=60 * 2**20),
        name="exchange",
    )(first, send, w_first, b_first[None], w_second, b_second[None], tok_rows.reshape(tok // GRP, GRP, width), w_route, expert_keys, tau.reshape(1, 1))


def combine_kernel(num_experts, final, meta_ref, back_ref, tail_ref, code_ref, prob_ref, o_ref, rows_in, sem):
    early = meta_ref[5, 0]
    first = early if final else 0
    i, last = pl.program_id(0), pl.num_programs(0) - 1
    span = WIN // GRP
    width = o_ref.shape[1]
    units = sem.shape[1]
    cols = lax.broadcasted_iota(jnp.int32, (BLK, 128), 1)
    row = lax.broadcasted_iota(jnp.int32, (WIN, width), 0)

    def unit(e, u, from_tail=False):
        part = pl.ds(u * UNIT, UNIT)
        return pltpu.make_async_copy(tail_ref.at[e] if from_tail else back_ref.at[e, part], rows_in.at[e, part], sem.at[e, u])

    def rows_before(step, e):
        n = step * STEP * num_experts + e
        return meta_ref[0, n] * GRP + meta_ref[3, n]

    def reach(step, e):
        return (rows_before(step, e) + (UNIT * GRP - 1)) // (UNIT * GRP)

    def block(k, carry):
        b = i * STEP + k
        mine = pl.ds(pl.multiple_of(k * BLK, BLK), BLK)
        code = jnp.transpose(jnp.broadcast_to(code_ref[pl.ds(b, 1), :], (128, BLK)))
        expert = (code & (num_experts * WIN - 1)) // WIN
        gate = jnp.sum(jnp.where(cols == expert, prob_ref[mine, :], 0.0), axis=1, keepdims=True)

        def picked(p):
            sel = jnp.concatenate([onehot(cols + k == code - p * (num_experts * WIN)) for k in range(0, num_experts * WIN, 128)], axis=1)
            wins = []
            for e in range(num_experts):
                at = jnp.minimum(meta_ref[0, b * num_experts + e] + p * span, rows_in.shape[1] - span)
                rows = rows_in[e, pl.ds(at, span)].reshape(WIN, width)
                end = meta_ref[0, b * num_experts + e] * GRP + meta_ref[4, b * num_experts + e]
                wins.append(jnp.where(row < end - at * GRP, rows, jnp.zeros_like(rows)))
            return jnp.dot(sel.astype(jnp.bfloat16), jnp.concatenate(wins, axis=0), preferred_element_type=jnp.float32)

        o_ref[mine, :] = (gate * picked(0)).astype(jnp.bfloat16)

        def more(p, carry):
            o_ref[mine, :] += (gate * picked(p)).astype(jnp.bfloat16)
            return carry

        return lax.fori_loop(1, most(meta_ref, b, num_experts), more, carry)

    @pl.when(i == first)
    def _():
        for u in range(units if final else units - 1):
            for e in range(num_experts):
                if final:
                    wanted = (u >= rows_before(early, e) // (UNIT * GRP)) & (u < used_units(meta_ref, e))
                else:
                    wanted = u < reach(early, e)

                @pl.when(wanted)
                def _():
                    unit(e, u, u == units - 1).start()

    @pl.when((i >= early) if final else (i < early))
    def _():
        for e in range(num_experts):
            begin = reach(i, e)
            end = reach(jnp.minimum(i + 1, last), e)
            if final:
                begin = jnp.where(i == early, rows_before(early, e) // (UNIT * GRP), begin)
                end = jnp.where(i == last, used_units(meta_ref, e), end)
            lax.fori_loop(begin, end, lambda u, c, e=e: (unit(e, u).wait(), c)[1], 0)
        lax.fori_loop(0, STEP, block, 0)


def combine(back, tail, code, meta, probs, out=None):
    tok, width = probs.shape[0], back.shape[3]
    num_experts, slot_groups = back.shape[:2]
    final = out is not None
    steps = tok // (BLK * STEP)
    kernel = functools.partial(combine_kernel, num_experts, final)
    hbm = pl.BlockSpec(memory_space=pl.ANY)

    def mine(i, meta_ref):
        return (jnp.maximum(i, meta_ref[5, 0]), 0) if final else (jnp.minimum(i, jnp.maximum(meta_ref[5, 0] - 1, 0)), 0)

    def call(meta_ref, *refs):
        if final:
            back_ref, tail_ref, code_ref, prob_ref, _, *rest = refs
        else:
            back_ref, code_ref, prob_ref, *rest = refs
            tail_ref = None
        kernel(meta_ref, back_ref, tail_ref, code_ref, prob_ref, *rest)

    table = pl.BlockSpec(code.shape, lambda i, *_: (0, 0))
    gates = pl.BlockSpec((STEP * BLK, 128), mine)
    return pl.pallas_call(
        call,
        grid_spec=pltpu.PrefetchScalarGridSpec(
            num_scalar_prefetch=1,
            grid=(steps,),
            in_specs=[hbm, hbm, table, gates, hbm] if final else [hbm, table, gates],
            out_specs=pl.BlockSpec((STEP * BLK, width), mine),
            scratch_shapes=[
                pltpu.VMEM((num_experts, slot_groups + WIN // GRP, GRP, width), jnp.bfloat16),
                pltpu.SemaphoreType.DMA((num_experts, slot_groups // UNIT)),
            ],
        ),
        out_shape=jax.ShapeDtypeStruct((tok, width), jnp.bfloat16),
        input_output_aliases={5: 0} if final else {},
        compiler_params=pltpu.CompilerParams(vmem_limit_bytes=63 * 2**20),
        cost_estimate=pl.CostEstimate(flops=2 * tok * num_experts * WIN * width, bytes_accessed=5 * tok * width, transcendentals=0),
        name="combine_final" if final else "combine",
    )(*((meta, back, tail, code, probs, out) if final else (meta, back, code, probs)))


def solution(mesh):
    num_experts = mesh.shape["ep_b"] * mesh.shape["ep_a"]
    tok_spec = P(("dp",) + EXPERT_AXES)
    expert_spec = P(EXPERT_AXES)

    def device_step(tokens, expert_ids, route_order, w_route, expert_keys, tau, w_in, b_in, w_out, b_out):
        tok_rows, id_row = tokens[0], expert_ids[0]
        tok, width = tok_rows.shape
        capacity = (5 * tok + 4 * num_experts - 1) // (4 * num_experts)
        slot_groups = -(-capacity // (GRP * UNIT * CHUNKS)) * UNIT * CHUNKS
        code, meta, first = route(route_order[0], id_row, tok_rows, num_experts, capacity)
        send = dispatch(tok_rows, code, meta, first, slot_groups)
        first = lax.all_to_all(first, EXPERT_AXES, 0, 0, tiled=True)
        back, _, _, tail, probs = exchange(first, send, w_in[0], b_in[0], w_out[0], b_out[0], tok_rows, w_route, expert_keys, tau)
        tail = lax.all_to_all(tail, EXPERT_AXES, 0, 0, tiled=True)
        out = combine(back, None, code, meta, probs)
        return combine(back, tail, code, meta, probs, out)[None]

    return jax.shard_map(
        device_step,
        mesh=mesh,
        in_specs=(tok_spec, tok_spec, tok_spec, P(), P(), P(), expert_spec, expert_spec, expert_spec, expert_spec),
        out_specs=tok_spec,
        check_vma=False,
    )
```
